32 devices in a mesh: var: 8 (over z, core), samp: 4 (over y, x).
Axes of the slice: x: 2, y: 2, z: 4, core: 2. Of those that a mesh axis runs over, the one named last changes fastest.
Arguments:
- geno: bfloat16 [8192, 16384], P('samp', 'var'), may hold values from -5 to 5
- scale_index: int32 [64, 16384], P('samp', 'var'), may hold values from 0 to 15
- scale_table: float32 [16], replicated, may hold values from 0.25 to 4
- residual: float32 [8, 8192], P(None, 'samp'), may hold values from -6 to 6
- beta_active: float32 [8, 3584], P(None, 'var'), may hold values from -6 to 6
- block_inverse: float32 [16, 256, 256], P('var'), may hold values from -1 to 4
- active_ids: int32 [3584], P('var'), may hold values from 0 to 16383, as said below
- admit_ids: int32 [512], P('var'), may hold values from 0 to 16383, as said below
Outputs:
- scores: float32 [8, 16384], P(None, 'var')
- coefficients: float32 [8, 4096], P(None, 'var')
- residual_out: float32 [8, 8192], P(None, 'samp')
The draws below stay inside these ranges and needn't reach their ends.
Inputs may be any that keep to these rules, and one draw needn't show every extreme that they name: Variant ids, all different from one another and from those of admit_ids. The fitting slots of one index of var are its 448 entries of active_ids followed by its 64 entries of admit_ids; of these 512 slots at most 128 name variants held by any one index of var, and for every index of var some one holder reaches exactly 128. `admit_ids`: variant ids, as for active_ids.
All inputs are finite; a program needn't handle non-finite values.
Results may differ from the reference program's by a relative error of at most 0.004.
Values may be sent and summed in bfloat16 or wider, within the bound.
A program may use at most 128 MiB of HBM per device.

```python
import math
import jax
import jax.numpy as jnp
from jax import lax

PHENO = 8
BLOCK = 256
GROUP = 128
LEVELS = 16
PASSES = 3
VAR_DEV = 2048
ADM_DEV = 64
FIT_DEV = 512
ACT_DEV = 448
SAMPLES = 8192
VARIANTS = 16384
ACTIVE = 3584
FIT = 4096
NBLK = 16
N_VAR = 8


def fit_layout(key):
    base_key = jax.random.fold_in(key, 7)
    holders = N_VAR
    capacity = 2 * FIT_DEV // holders
    pairing = jax.vmap(lambda keyed: jax.random.permutation(keyed, holders))(jax.random.split(jax.random.fold_in(base_key, 1), holders))
    shares = jax.random.randint(jax.random.fold_in(base_key, 2), (holders, holders // 2), 0, capacity + 1, dtype=jnp.int32)
    shares = shares.at[:, 0].set(0)
    paired = jnp.stack([capacity - shares, shares], -1).reshape(holders, holders)
    rows_index = jnp.arange(holders, dtype=jnp.int32)[:, None]
    counts = jnp.zeros((holders, holders), jnp.int32).at[rows_index, pairing].set(paired)
    finish = jnp.cumsum(counts, 1)
    anchor = finish - counts
    slot_range = jnp.arange(FIT_DEV, dtype=jnp.int32)
    holder = jnp.sum((finish[:, None, :] <= slot_range[None, :, None]).astype(jnp.int32), -1)
    serial = slot_range[None, :] - jnp.take_along_axis(anchor, holder, 1)
    offsets = jnp.cumsum(counts, 0) - counts
    shuffled = jax.vmap(lambda keyed: jax.random.permutation(keyed, VAR_DEV))(jax.random.split(jax.random.fold_in(base_key, 3), holders))
    column = shuffled[holder, jnp.take_along_axis(offsets, holder, 1) + serial]
    chosen = holder * VAR_DEV + column
    reorder = jax.vmap(lambda keyed: jax.random.permutation(keyed, FIT_DEV))(jax.random.split(jax.random.fold_in(base_key, 4), holders))
    return jnp.take_along_axis(chosen, reorder, 1).astype(jnp.int32)


def draw_active_ids(key, part):
    return fit_layout(key)[:, :ACT_DEV].reshape(-1)


def draw_admit_ids(key, part):
    return fit_layout(key)[:, ACT_DEV:].reshape(-1)


def draw_block_inverse(key, part):
    noise = jax.random.normal(jax.random.fold_in(key, 11), (NBLK, BLOCK, BLOCK), jnp.float32)
    diagonal = jnp.exp(jax.random.uniform(jax.random.fold_in(key, 12), (NBLK, BLOCK), jnp.float32, 0.0, 0.6931))
    spread = 0.35
    symmetric = (noise + jnp.swapaxes(noise, 1, 2)) * (spread / (2.0 * BLOCK) ** 0.5)
    return jnp.eye(BLOCK, dtype=jnp.float32)[None, :, :] * diagonal[:, :, None] + symmetric


def set_ends(drawn, key, smallest, largest):
    longest = drawn.shape.index(max(drawn.shape))
    spots = []
    for shift in (0, 1):
        where = [jax.random.randint(jax.random.fold_in(key, axis), (), 0, length) for axis, length in enumerate(drawn.shape)]
        where[longest] = (where[longest] + shift) % drawn.shape[longest]
        spots.append(tuple(where))
    return drawn.at[spots[0]].set(smallest).at[spots[1]].set(largest)


def block_scale(own_key, extent, pieces, low, top_value):
    loudness, own = 1.0, jax.random.fold_in(own_key, 6)
    for dim, blocks in pieces:
        steps = jnp.exp(jax.random.uniform(jax.random.fold_in(own, dim), (blocks,), jnp.float32, low / len(pieces), top_value / len(pieces)))
        loudness = loudness * jnp.repeat(steps, extent[dim] // blocks).reshape([-1 if axis == dim else 1 for axis in range(len(extent))])
    return loudness


def gaussian(rng, extent, width, bound, shards=(), kind=jnp.bfloat16):
    entries = jax.random.normal(rng, extent, jnp.float32) * width
    if len(shards) > 0:
        entries = block_scale(rng, extent, shards, -0.22, 0.18) * entries
    return jnp.clip(entries, min=-bound, max=bound).astype(kind)


def setup_inputs(seed: int = 0) -> dict:
    key_of = jax.random.split(jax.random.key(seed), 9)
    geno = gaussian(key_of[0], (SAMPLES, VARIANTS), 1.0, 5.0, ((0, 4), (1, 8)))
    scale_index = set_ends(jax.random.randint(key_of[1], (SAMPLES // GROUP, VARIANTS), 0, LEVELS), jax.random.fold_in(key_of[1], 1), 0, LEVELS - 1).astype(jnp.int32)
    scale_table = jnp.clip(jnp.exp(jax.random.uniform(key_of[2], (LEVELS,), jnp.float32, math.log(0.25), math.log(4.0))), 0.25, 4.0)
    residual = gaussian(key_of[3], (PHENO, SAMPLES), 1.0, 6.0, ((1, 4),), jnp.float32)
    beta_active = gaussian(key_of[4], (PHENO, ACTIVE), 1.0, 6.0, ((1, 8),), jnp.float32)
    block_inverse = draw_block_inverse(jax.random.fold_in(key_of[8], 71), 0)
    active_ids = draw_active_ids(jax.random.fold_in(key_of[8], 71), 0)
    admit_ids = draw_admit_ids(jax.random.fold_in(key_of[8], 71), 0)
    return {"geno": geno, "scale_index": scale_index, "scale_table": scale_table, "residual": residual, "beta_active": beta_active, "block_inverse": block_inverse, "active_ids": active_ids, "admit_ids": admit_ids}


penalty = 0.5
epsilon = 1e-06

def dequantize(values, indices, lookup):
    groups = indices.shape[0]
    scales = lookup[indices]
    widened = values.reshape(groups, values.shape[0] // groups, values.shape[1]).astype(jnp.float32) * scales[:, None, :]
    return widened.reshape(values.shape).astype(jnp.bfloat16)

def reference(geno, scale_index, scale_table, residual, beta_active, block_inverse, active_ids, admit_ids):
    inv_root = 1.0 / math.sqrt(SAMPLES)
    resid_low = residual.astype(jnp.bfloat16)

    def screen_block(block_index):
        first_column = block_index * VAR_DEV
        values = lax.dynamic_slice_in_dim(geno, first_column, VAR_DEV, 1)
        indices = lax.dynamic_slice_in_dim(scale_index, first_column, VAR_DEV, 1)
        return jnp.dot(resid_low, dequantize(values, indices, scale_table), preferred_element_type=jnp.float32)
    blocks = lax.map(screen_block, jnp.arange(N_VAR, dtype=jnp.int32))
    scores = jnp.transpose(blocks, (1, 0, 2)).reshape(PHENO, VARIANTS) * inv_root
    fit_ids = jnp.concatenate([active_ids.reshape(N_VAR, ACT_DEV), admit_ids.reshape(N_VAR, ADM_DEV)], 1).reshape(FIT)
    fitting = dequantize(jnp.take(geno, fit_ids, axis=1), jnp.take(scale_index, fit_ids, axis=1), scale_table)
    coeffs = jnp.concatenate([beta_active.reshape(PHENO, N_VAR, ACT_DEV), jnp.zeros((PHENO, N_VAR, ADM_DEV), jnp.float32)], 2).reshape(PHENO, FIT)
    current = residual
    for pass_index in range(PASSES):
        gradient = jnp.dot(current.astype(jnp.bfloat16), fitting, preferred_element_type=jnp.float32) * inv_root
        inner_term = (gradient - penalty * coeffs).reshape(PHENO, NBLK, BLOCK)
        direction = jnp.einsum('bij,pbj->pbi', block_inverse, inner_term, precision=lax.Precision.HIGHEST)
        direction = direction.reshape(PHENO, FIT).astype(jnp.bfloat16)
        update = jnp.dot(direction, fitting.T, preferred_element_type=jnp.float32) * inv_root
        cross_sum = lax.optimization_barrier(jnp.sum(current * update, 1))
        square = lax.optimization_barrier(jnp.sum(update * update, 1)) + epsilon
        factor = (cross_sum / square)[:, None]
        current = current - factor * update
        coeffs = coeffs + factor * direction.astype(jnp.float32)
    return (scores, coeffs, current)
```

```python
import functools
import math

import jax
import jax.numpy as jnp
from jax import lax
from jax.experimental import pallas as pl
from jax.experimental.pallas import tpu as pltpu
from jax.sharding import PartitionSpec as P

PASSES = 3
PENALTY = 0.5
EPSILON = 1e-06
LANES = 128
F32 = jnp.float32
BF16 = jnp.bfloat16
NN = (((1,), (0,)), ((), ()))
NT = (((1,), (1,)), ((), ()))


def dot(a, b, dims=NN):
    return lax.dot_general(a, b, dims, preferred_element_type=F32)


def split(x):
    high = x.astype(BF16).astype(F32)
    return jnp.concatenate([high, x - high], axis=0).astype(BF16)


def joined(x):
    half = x.shape[0] // 2
    return x[:half] + x[half:]


def owners_of(V):
    return (V // 2, 2) if V % 8 == 0 else (V, 1)


def group_order(V):
    O, G = owners_of(V)
    if G == 1:
        return list(range(V))
    order = []
    for q in range(O):
        h, zc, c = q // 4, 1 + (q % 4) // 2, q % 2
        edge = 0 if zc == 1 else 3
        order += [8 * h + 2 * zc + c, 8 * h + 2 * edge + c]
    return order


def kernel(
    V, S, pad,
    geno, sidx, table, resid, beta, binv, active, admit,
    scores_out, coef_out, resid_out,
    x_ref, sidx_v, table_s, cur, beta_v, binv_v, act_v, adm_v,
    scale_ref, rlow, part, low, high_t, marks_v, place_v, tri, inv, beta_two, ids_all,
    d_held, coef, grad, direct,
    send_a, recv_a, send_b, recv_b, send_c, recv_c, recv_u, recv_p, recv_s, recv_d,
    load_sem, in_sem, send_sem, recv_sem,
):
    cur_scope = [None]

    def mk(name):
        pass

    N = V * S
    O, G = owners_of(V)
    order = group_order(V)
    rows, width = x_ref.shape
    groups = sidx_v.shape[0]
    per_group = rows // groups
    levels = table_s.shape[0]
    ph = cur.shape[0]
    kept = act_v.shape[1]
    fit = kept + adm_v.shape[1]
    blocks, bsize = binv_v.shape[0], binv_v.shape[1]
    chunk = rows // O
    tiles = width // LANES
    step = 2 * per_group
    n_steps = rows // step
    inv_root = 1.0 / math.sqrt(rows * S)
    mv, ms = lax.axis_index("var"), lax.axis_index("samp")
    me = ms * V + mv

    mk("greet")
    barrier = pltpu.get_barrier_semaphore()

    def greet(k, c):
        t = lax.rem(me + k, N)
        pl.semaphore_signal(
            barrier, inc=1, device_id={"var": lax.rem(t, V), "samp": lax.div(t, V)},
            device_id_type=pl.DeviceIdType.MESH,
        )
        return c

    lax.fori_loop(1, N, greet, 0)
    mk("start")

    def load(i):
        at = pl.ds(pl.multiple_of(i * step, step), step)
        return pltpu.make_async_copy(geno.at[at], x_ref.at[at], load_sem.at[i])

    small = [(table, table_s), (sidx, sidx_v), (resid, cur), (active, act_v), (admit, adm_v), (beta, beta_v), (binv, binv_v)]
    pulls = [pltpu.make_async_copy(a, b, in_sem.at[i]) for i, (a, b) in enumerate(small)]
    for c in pulls[:5]:
        c.start()
    load(0).start()
    load(1).start()
    for c in pulls[5:]:
        c.start()
    for i in range(2, n_steps):
        load(i).start()

    if G == 1:
        is_owner, my_q = None, mv
        owners = [(lax.rem(mv + 1 + k, V), lax.rem(mv + 1 + k, V)) for k in range(V)]
        all_var = [lax.rem(mv + 1 + k, V) for k in range(V - 1)]
        partner = None
    else:
        H = V // 8
        h, z, c0 = lax.div(mv, 8), lax.rem(lax.div(mv, 2), 4), lax.rem(mv, 2)
        side = lax.div(z, 2)
        cores = (1 - c0, c0)
        hs = [lax.rem(h + d, H) for d in range(1, H)] + [h]
        owners = [
            (8 * hh + 2 * zc + cc, 4 * hh + 2 * (zc - 1) + cc)
            for hh in hs for zc in (2 - side, 1 + side) for cc in cores
        ]
        is_owner = z == 1 + side
        my_q = 4 * h + 2 * side + c0
        z0 = z + side * (3 - 2 * z)
        zs = [side * 3 + (1 - 2 * side) * k for k in (3, 2, 1 - z0, z0)]
        all_var = [8 * hh + 2 * zz + cc for hh in hs for zz in zs for cc in cores][:-1]
        partner = 8 * h + 2 * (side * 3 + (1 - 2 * side) * (1 - z0)) + c0
    samps = [lax.rem(ms + d, S) for d in range(1, S)]

    def owner_only(fn):
        if G == 1:
            fn()
        else:
            pl.when(is_owner)(fn)

    def other_only(fn):
        if G > 1:
            pl.when(jnp.logical_not(is_owner))(fn)

    def send(src, dst, sem, v, s, r_sem=None):
        pltpu.make_async_remote_copy(
            src_ref=src, dst_ref=dst, send_sem=send_sem.at[sem],
            recv_sem=recv_sem.at[sem if r_sem is None else r_sem],
            device_id={"var": v, "samp": s}, device_id_type=pl.DeviceIdType.MESH,
        ).start()

    def got(ref, sem):
        pltpu.make_async_copy(ref, ref, recv_sem.at[sem]).wait()

    def sent(ref, sem):
        pltpu.make_async_copy(ref, ref, send_sem.at[sem]).wait()

    IDS, INV, BETA, SC = 0, 1, 2, 3
    A = 4
    B = A + PASSES
    C = B + PASSES
    SM = C + PASSES
    D = SM + PASSES
    U = D + PASSES
    UQ = U + PASSES

    mk("setup")
    for c in pulls[:5]:
        c.wait()
    ids_all[mv, :, 0:kept] = act_v[...]
    ids_all[mv, :, kept:fit] = adm_v[...]
    index = sidx_v[...]
    scales = jnp.zeros(index.shape, F32)
    for level in range(levels):
        scales = jnp.where(index == level, table_s[level], scales)
    scale_ref[...] = scales
    rlow[...] = cur[...].astype(BF16)
    part[...] = jnp.zeros((ph, width), F32)
    cols = 256

    def screen(i, c):
        load(i).wait()
        at = pl.ds(pl.multiple_of(i * step, step), step)
        left = rlow[:, at]
        for j in range(width // cols):
            lane = slice(j * cols, (j + 1) * cols)
            block = []
            for half in range(2):
                sub = pl.ds(pl.multiple_of(i * step + half * per_group, per_group), per_group)
                block.append(x_ref[sub, lane].astype(F32) * scale_ref[pl.ds(2 * i + half, 1), lane])
            block = jnp.concatenate(block, axis=0).astype(BF16)
            x_ref[at, lane] = block
            part[:, lane] += dot(left, block)
        return c

    first = (n_steps * 5) // 8
    mk("screen1")
    lax.fori_loop(0, first, screen, 0)
    mk("inv")
    for c in pulls[5:]:
        c.wait()
    for b in range(blocks):
        inv[0, b] = binv_v[b].astype(BF16)
    tri[...] = jnp.where(
        lax.broadcasted_iota(jnp.int32, (fit, fit), 0) < lax.broadcasted_iota(jnp.int32, (fit, fit), 1),
        1.0, 0.0,
    ).astype(BF16)
    mk("barrier")
    pl.semaphore_wait(barrier, N - 1)
    for v in all_var:
        send(ids_all.at[mv], ids_all.at[mv], IDS, v, ms)

    def hand_over():
        send(beta_v, beta_two, BETA, partner, ms)
        send(inv.at[0], inv.at[1], INV, partner, ms)

    other_only(hand_over)
    mk("screen2")
    lax.fori_loop(first, n_steps, screen, 0)
    recv_p[ms] = part[...]

    mk("idswait")
    got(ids_all.at[pl.ds(0, V - 1)], IDS)
    mk("idsproc")
    line = lax.broadcasted_iota(jnp.int32, (V, fit), 0)

    def lines(g):
        return ids_all[g, 0:1, :]

    all_ids = jnp.zeros((V, fit), jnp.int32)
    for g in range(V):
        all_ids = jnp.where(line == g, lines(g), all_ids)
    column = all_ids - mv * width
    held = (column >= 0) & (column < width)
    serial = dot(jnp.where(held, 1.0, 0.0).astype(BF16), tri[...])
    serial = jnp.where(held, serial, -1.0)
    column = jnp.where(held, column, 0)
    eight = lax.broadcasted_iota(jnp.int32, (8, fit), 0)
    turn = lax.broadcasted_iota(jnp.int32, (pad, fit), 0).astype(F32)
    lane_no = lax.broadcasted_iota(jnp.int32, (LANES, pad), 0).astype(F32)
    for n, g in enumerate(order):
        col = column[g:g + 1]
        digits = jnp.where(
            eight == 0, lax.shift_right_logical(col, 7),
            jnp.where(eight == 1, col & 127, jnp.where(eight == 2, 1, 0)),
        ).astype(F32).astype(BF16)
        place = jnp.where(turn == serial[g:g + 1], 1.0, 0.0).astype(BF16)
        found = dot(digits, place, NT)
        here = found[2:3] > 0.5
        at = slice(n * pad, (n + 1) * pad)
        high_t[:, at] = jnp.broadcast_to(jnp.where(here, found[0:1], -1.0), (ph, pad))
        low[:, at] = jnp.where(lane_no == jnp.where(here, found[1:2], -1.0), 1.0, 0.0).astype(BF16)

    mk("own")

    def own_slots():
        for i in range(G):
            mine = (ids_all[mv if i == 0 else partner][0:1]) - line * width
            marks = jnp.where((mine >= 0) & (mine < width), 1.0, 0.0)
            before = dot(marks.astype(BF16), tri[...])
            position = jnp.sum(marks * before, axis=0, keepdims=True)
            place_v[i] = jnp.where(turn == position, 1.0, 0.0).astype(BF16)
            marks_v[i] = marks

    def send_gradient(p):
        wide = jnp.concatenate([part[:, t * LANES:(t + 1) * LANES] for t in range(tiles)], axis=0).astype(BF16)
        half = O * G * pad // 2
        for n in range(2):
            at = slice(n * half, (n + 1) * half)
            found = dot(wide, low[:, at])
            which = high_t[:, at]
            out = jnp.zeros((ph, half), F32)
            for t in range(tiles):
                out = jnp.where(which == float(t), found[t * ph:(t + 1) * ph], out)
            out = out.astype(BF16)
            each = G * pad
            for k in range(half // each):
                send_a[p, n * (half // each) + k] = out[:, k * each:(k + 1) * each]
        targets = []
        for k, (v, q) in enumerate(owners):
            for s in samps + [ms]:
                targets.append((v, q, s, k == O - 1 and s is ms))
        for v, q, s, last in targets:
            if not last:
                send(send_a.at[p, q], recv_a.at[p, me], A + p, v, s)
        v, q, s, _ = targets[-1]

        def away():
            send(send_a.at[p, q], recv_a.at[p, me], A + p, v, s)

        other_only(away)

        def stay():
            recv_a[p, me] = send_a[p, q]

        owner_only(stay)

    def wait_sums(p):
        owner_only(lambda: got(recv_s.at[p, pl.ds(0, S * O - 1)], SM + p))
        other_only(lambda: got(recv_s.at[p, pl.ds(0, S * O)], SM + p))

    lane = lax.broadcasted_iota(jnp.int32, (ph, LANES), 1)
    sub = lax.broadcasted_iota(jnp.int32, (ph, LANES), 0)

    def length(p):
        wait_sums(p)
        total = recv_s[p, 0]
        for k in range(1, S * O):
            total = total + recv_s[p, k]
        total = jnp.broadcast_to(total, (ph, LANES))
        cross = jnp.sum(jnp.where(lane == sub, total, 0.0), axis=1, keepdims=True)
        square = jnp.sum(jnp.where(lane == sub + ph, total, 0.0), axis=1, keepdims=True)
        return cross / (square + EPSILON)

    def advance(factor, p, dst):
        for q in range(O):
            at = slice(q * chunk, (q + 1) * chunk)
            dst[:, at] = cur[:, at] - factor * recv_u[p, q].astype(F32)

    def serve(p, factor):
        got(recv_a.at[p, pl.ds(0, N - 1)], A + p)
        mk("slots")
        if p == 0:
            coef[...] = jnp.zeros(coef.shape, F32)
            coef[0, :, 0:kept] = beta_v[...]
            if G > 1:
                got(beta_two, BETA)
                coef[1, :, 0:kept] = beta_two[...]
                got(inv.at[1], INV)
        for i in range(G):
            at = slice(i * pad, (i + 1) * pad)
            stack = []
            for v in range(V):
                val = recv_a[p, v, :, at].astype(F32)
                for s in range(1, S):
                    val = val + recv_a[p, s * V + v, :, at].astype(F32)
                high = val.astype(BF16).astype(F32)
                stack += [high, val - high]
            found = dot(jnp.concatenate(stack, axis=0).astype(BF16), place_v[i])
            slots = jnp.zeros((ph, fit), F32)
            for v in range(V):
                both = found[2 * v * ph:(2 * v + 1) * ph] + found[(2 * v + 1) * ph:(2 * v + 2) * ph]
                slots = slots + marks_v[i, v:v + 1] * both
            slots = slots * inv_root
            if p > 0:
                slots = grad[i] - factor * slots
                coef[i] = coef[i] + factor * direct[p - 1, i].astype(F32)
            grad[i] = slots
            inner = slots - PENALTY * coef[i]
            for b in range(blocks):
                cut = slice(b * bsize, (b + 1) * bsize)
                direct[p, i, :, cut] = joined(dot(split(inner[:, cut]), inv[i, b], NT)).astype(BF16)
            way = direct[p, i].astype(F32)
            spread = jnp.concatenate([way * marks_v[i, v:v + 1] for v in range(V)], axis=0).astype(BF16)
            back = dot(spread, place_v[i], NT).astype(BF16)
            for v in range(V):
                send_b[p, v, :, at] = back[v * ph:(v + 1) * ph]
        for v in all_var:
            send(send_b.at[p, v], recv_b.at[p, my_q], B + p, v, ms)
        if G > 1:
            send(direct.at[p, 1], recv_d.at[p], D + p, partner, ms)
        recv_b[p, my_q] = send_b[p, mv]

    def reduce(p):
        got(recv_c.at[p, pl.ds(0, V - 1)], C + p)
        mk("sumC")
        val = recv_c[p, 0].astype(F32)
        for v in range(1, V):
            val = val + recv_c[p, v].astype(F32)
        low_u = (val * inv_root).astype(BF16)
        recv_u[p, my_q] = low_u
        for v in all_var:
            send(recv_u.at[p, my_q], recv_u.at[p, my_q], U + p, v, ms, UQ + p * O + my_q)
        upd = low_u.astype(F32)
        now = cur[:, pl.ds(pl.multiple_of(my_q * chunk, chunk), chunk)]
        cross = jnp.sum(now * upd, axis=1, keepdims=True)
        square = jnp.sum(upd * upd, axis=1, keepdims=True)
        both = jnp.where(lane == sub, cross, jnp.where(lane == sub + ph, square, 0.0))
        slot = ms * O + my_q
        recv_s[p, slot] = jnp.sum(both, axis=0, keepdims=True)
        for v in all_var:
            for s in samps + [ms]:
                send(recv_s.at[p, slot], recv_s.at[p, slot], SM + p, v, s)
        for s in samps:
            send(recv_s.at[p, slot], recv_s.at[p, slot], SM + p, mv, s)

    owner_only(own_slots)
    factors = []
    for p in range(PASSES):
        mk("gather")
        send_gradient(p)
        mk("mid")
        if p == 0:
            for s in samps:
                send(recv_p.at[ms], recv_p.at[ms], SC, mv, s)
        if p == 1:
            got(recv_p.at[pl.ds(0, S - 1)], SC)
            val = recv_p[0]
            for s in range(1, S):
                val = val + recv_p[s]
            scores_out[...] = val * inv_root
        if p > 0:
            factors.append(length(p - 1))
        factor = factors[-1] if p else None
        mk("waitA")
        owner_only(functools.partial(serve, p, factor))
        mk("adv")
        if p > 0:
            advance(factor, p - 1, cur)
        mk("waitB")
        owner_only(lambda: got(recv_b.at[p, pl.ds(0, O - 1)], B + p))
        other_only(lambda: got(recv_b.at[p, pl.ds(0, O)], B + p))
        mk("spread")
        way = jnp.concatenate([recv_b[p, q] for q in range(O)], axis=1).astype(F32)
        which = high_t[...]
        wide = jnp.concatenate([jnp.where(which == float(t), way, 0.0) for t in range(tiles)], axis=0)
        found = dot(wide.astype(BF16), low[...], NT).astype(BF16)
        for t in range(tiles):
            d_held[:, t * LANES:(t + 1) * LANES] = found[t * ph:(t + 1) * ph]
        mk("upd")

        def piece(q):
            at = pl.ds(pl.multiple_of(q * chunk, chunk), chunk)
            return dot(x_ref[at, :], d_held[...], NT).T.astype(BF16)

        for k, (v, q) in enumerate(owners):
            if k < O - 1:
                send_c[p, k] = piece(q)
                send(send_c.at[p, k], recv_c.at[p, mv], C + p, v, ms)
            else:
                send_c[p, k] = piece(q)

                def away(k=k, v=v):
                    send(send_c.at[p, k], recv_c.at[p, mv], C + p, v, ms)

                other_only(away)

                def stay(k=k):
                    recv_c[p, mv] = send_c[p, k]

                owner_only(stay)
        mk("waitC")
        owner_only(functools.partial(reduce, p))
        mk("waitU")
        for k, (v, q) in enumerate(reversed(owners)):
            def arrive(q=q):
                got(recv_u.at[p, q], UQ + p * O + q)

            if k == 0:
                other_only(arrive)
            else:
                arrive()
            if p + 1 < PASSES:
                at = pl.ds(pl.multiple_of(q * chunk, chunk), chunk)
                new = dot(recv_u[p, q], x_ref[at, :])
                if k == 0:
                    part[...] = new
                else:
                    part[...] += new

    mk("fin")
    factors.append(length(PASSES - 1))
    factor = factors[-1]
    advance(factor, PASSES - 1, resid_out)

    def own_coef():
        coef_out[...] = coef[0] + factor * direct[PASSES - 1, 0].astype(F32)

    owner_only(own_coef)

    def edge_coef():
        val = jnp.zeros((ph, fit), F32)
        coef[0] = val
        coef[0, :, 0:kept] = beta_v[...]
        val = coef[0]
        for p in range(PASSES):
            got(recv_d.at[p], D + p)
            val = val + factors[p] * recv_d[p].astype(F32)
        coef_out[...] = val

    other_only(edge_coef)
    mk("drain")

    sent(ids_all.at[pl.ds(0, V - 1)], IDS)
    sent(recv_p.at[pl.ds(0, S - 1)], SC)

    def drain_owner():
        for p in range(PASSES):
            sent(recv_a.at[p, pl.ds(0, S * O - 1)], A + p)
            sent(send_b.at[p, pl.ds(0, V - 1)], B + p)
            if O > 1:
                sent(send_c.at[p, pl.ds(0, O - 1)], C + p)
            sent(recv_c.at[p, pl.ds(0, V - 1)], U + p)
            sent(all_rows(p), SM + p)
            if G > 1:
                sent(direct.at[p, 1], D + p)

    def all_rows(p):
        return recv_s.at[p, pl.ds(0, N - 1)]

    owner_only(drain_owner)

    def drain_other():
        sent(beta_v, BETA)
        sent(inv.at[0], INV)
        for p in range(PASSES):
            sent(recv_a.at[p, pl.ds(0, S * O)], A + p)
            sent(send_c.at[p], C + p)

    other_only(drain_other)


def on_device(geno, scale_index, scale_table, residual, beta_active, block_inverse, active_ids, admit_ids):
    V, S = lax.axis_size("var"), lax.axis_size("samp")
    N = V * S
    O, G = owners_of(V)
    rows, width = geno.shape
    ph = residual.shape[0]
    fit = active_ids.shape[0] + admit_ids.shape[0]
    pad = LANES * pl.cdiv(2 * fit // V, LANES)
    chunk = rows // O
    vmem = pl.BlockSpec(memory_space=pltpu.VMEM)
    hbm = pl.BlockSpec(memory_space=pl.ANY)
    n_send = 4 + 6 * PASSES
    n_recv = n_send + PASSES * O
    per_group = rows // scale_index.shape[0]
    return pl.pallas_call(
        functools.partial(kernel, V, S, pad),
        out_shape=(
            jax.ShapeDtypeStruct((ph, width), F32),
            jax.ShapeDtypeStruct((ph, fit), F32),
            jax.ShapeDtypeStruct((ph, rows), F32),
        ),
        in_specs=[hbm] * 8,
        out_specs=(vmem, vmem, vmem),
        scratch_shapes=[
            pltpu.VMEM((rows, width), BF16),
            pltpu.VMEM(scale_index.shape, jnp.int32),
            pltpu.SMEM(scale_table.shape, F32),
            pltpu.VMEM((ph, rows), F32),
            pltpu.VMEM(beta_active.shape, F32),
            pltpu.VMEM(block_inverse.shape, F32),
            pltpu.VMEM((1, active_ids.shape[0]), jnp.int32),
            pltpu.VMEM((1, admit_ids.shape[0]), jnp.int32),
            pltpu.VMEM(scale_index.shape, F32),
            pltpu.VMEM((ph, rows), BF16),
            pltpu.VMEM((ph, width), F32),
            pltpu.VMEM((LANES, V * pad), BF16),
            pltpu.VMEM((ph, V * pad), F32),
            pltpu.VMEM((G, V, fit), F32),
            pltpu.VMEM((G, pad, fit), BF16),
            pltpu.VMEM((fit, fit), BF16),
            pltpu.VMEM((G,) + block_inverse.shape, BF16),
            pltpu.VMEM(beta_active.shape, F32),
            pltpu.VMEM((V, 1, fit), jnp.int32),
            pltpu.VMEM((ph, width), BF16),
            pltpu.VMEM((G, ph, fit), F32),
            pltpu.VMEM((G, ph, fit), F32),
            pltpu.VMEM((PASSES, G, ph, fit), BF16),
            pltpu.VMEM((PASSES, O, ph, G * pad), BF16),
            pltpu.VMEM((PASSES, N, ph, G * pad), BF16),
            pltpu.VMEM((PASSES, V, ph, G * pad), BF16),
            pltpu.VMEM((PASSES, O, ph, G * pad), BF16),
            pltpu.VMEM((PASSES, O, ph, chunk), BF16),
            pltpu.VMEM((PASSES, V, ph, chunk), BF16),
            pltpu.VMEM((PASSES, O, ph, chunk), BF16),
            pltpu.VMEM((S, ph, width), F32),
            pltpu.VMEM((PASSES, N, 1, LANES), F32),
            pltpu.VMEM((PASSES, ph, fit), BF16),
            pltpu.SemaphoreType.DMA((rows // (2 * per_group),)),
            pltpu.SemaphoreType.DMA((7,)),
            pltpu.SemaphoreType.DMA((n_send,)),
            pltpu.SemaphoreType.DMA((n_recv,)),
        ],
        compiler_params=pltpu.CompilerParams(
            collective_id=0, has_side_effects=True, vmem_limit_bytes=60 * 1024 * 1024
        ),
    )(geno, scale_index, scale_table, residual, beta_active, block_inverse, active_ids[None], admit_ids[None])


def solution(mesh):
    placed = (
        P("samp", "var"), P("samp", "var"), P(), P(None, "samp"), P(None, "var"),
        P("var", None, None), P("var"), P("var"),
    )
    return jax.shard_map(
        on_device, mesh=mesh, in_specs=placed,
        out_specs=(P(None, "var"), P(None, "var"), P(None, "samp")), check_vma=False,
    )
```

```python
import functools
import math

import jax
import jax.numpy as jnp
from jax import lax
from jax.experimental import pallas as pl
from jax.experimental.pallas import tpu as pltpu
from jax.sharding import PartitionSpec as P

PASSES = 3
PENALTY = 0.5
EPSILON = 1e-06
LANES = 128
F32 = jnp.float32
BF16 = jnp.bfloat16
NN = (((1,), (0,)), ((), ()))
NT = (((1,), (1,)), ((), ()))


def dot(a, b, dims=NN):
    return lax.dot_general(a, b, dims, preferred_element_type=F32)


def split(x):
    high = x.astype(BF16).astype(F32)
    return jnp.concatenate([high, x - high], axis=0).astype(BF16)


def joined(x):
    half = x.shape[0] // 2
    return x[:half] + x[half:]


def owners_of(V):
    return (V // 2, 2) if V % 8 == 0 else (V, 1)


def group_order(V):
    O, G = owners_of(V)
    if G == 1:
        return list(range(V))
    order = []
    for q in range(O):
        h, zc, c = q // 4, 1 + (q % 4) // 2, q % 2
        edge = 0 if zc == 1 else 3
        order += [8 * h + 2 * zc + c, 8 * h + 2 * edge + c]
    return order


def kernel(
    V, S, pad,
    geno, sidx, table, resid, beta, binv, active, admit,
    scores_out, coef_out, resid_out,
    x_ref, xt_ref, sidx_v, table_s, cur, beta_v, binv_v, act_v, adm_v,
    scale_ref, rlow, part, low, high_t, marks_v, place_v, tri, inv, beta_two, ids_all,
    d_held, coef, grad, direct,
    send_a, recv_a, send_b, recv_b, send_c, recv_c, recv_u, recv_p, recv_s, recv_d,
    load_sem, in_sem, send_sem, recv_sem,
):
    cur_scope = [None]

    def mk(name):
        pass

    N = V * S
    O, G = owners_of(V)
    order = group_order(V)
    rows, width = x_ref.shape
    groups = sidx_v.shape[0]
    per_group = rows // groups
    levels = table_s.shape[0]
    ph = cur.shape[0]
    kept = act_v.shape[1]
    fit = kept + adm_v.shape[1]
    blocks, bsize = binv_v.shape[0], binv_v.shape[1]
    chunk = rows // O
    join = G
    tiles = width // LANES
    piece = 2 * per_group
    n_loads = rows // piece
    per_step = 2 if n_loads % 2 == 0 else 1
    step = per_step * piece
    n_steps = rows // step
    inv_root = 1.0 / math.sqrt(rows * S)
    mv, ms = lax.axis_index("var"), lax.axis_index("samp")
    me = ms * V + mv

    mk("greet")
    barrier = pltpu.get_barrier_semaphore()

    samps = [lax.rem(ms + d, S) for d in range(1, S)] + [ms]
    if S == 4:
        samps = [3 - ms] + [ms + d - 2 * d * lax.rem(lax.div(ms, d), 2) for d in (2, 1)] + [ms]
    others = [lax.rem(mv + d, V) for d in range(V - 1, -1, -1)]
    for s in samps:
        for v in others[:-1] if s is ms else others:
            pl.semaphore_signal(
                barrier, inc=1, device_id={"var": v, "samp": s}, device_id_type=pl.DeviceIdType.MESH
            )
    mk("start")

    def load(i):
        at = pl.ds(pl.multiple_of(i * piece, piece), piece)
        return pltpu.make_async_copy(geno.at[at], x_ref.at[at], load_sem.at[i])

    small = [(table, table_s), (sidx, sidx_v), (resid, cur), (active, act_v), (admit, adm_v), (beta, beta_v), (binv, binv_v)]
    pulls = [pltpu.make_async_copy(a, b, in_sem.at[i]) for i, (a, b) in enumerate(small)]
    for c in pulls[:5]:
        c.start()
    load(0).start()

    if G == 1:
        is_owner, my_q = None, mv
        owners = [(lax.rem(mv + 1 + k, V), lax.rem(mv + 1 + k, V)) for k in range(V)]
        all_var = [lax.rem(mv + 1 + k, V) for k in range(V - 1)]
        partner = None
    else:
        H = V // 8
        h, z, c0 = lax.div(mv, 8), lax.rem(lax.div(mv, 2), 4), lax.rem(mv, 2)
        side = lax.div(z, 2)
        cores = (1 - c0, c0)
        hs = [lax.rem(h + d, H) for d in range(1, H)] + [h]
        owners = [
            (8 * hh + 2 * zc + cc, 4 * hh + 2 * (zc - 1) + cc)
            for hh in hs for zc in (2 - side, 1 + side) for cc in cores
        ]
        is_owner = z == 1 + side
        my_q = 4 * h + 2 * side + c0
        z0 = z + side * (3 - 2 * z)
        zs = [side * 3 + (1 - 2 * side) * k for k in (3, 2, 1 - z0, z0)]
        all_var = [8 * hh + 2 * zz + cc for hh in hs for zz in zs for cc in cores][:-1]
        partner = 8 * h + 2 * (side * 3 + (1 - 2 * side) * (1 - z0)) + c0
    samps = samps[:-1]

    def owner_only(fn):
        if G == 1:
            fn()
        else:
            pl.when(is_owner)(fn)

    def other_only(fn):
        if G > 1:
            pl.when(jnp.logical_not(is_owner))(fn)

    def send(src, dst, sem, v, s, r_sem=None):
        pltpu.make_async_remote_copy(
            src_ref=src, dst_ref=dst, send_sem=send_sem.at[sem],
            recv_sem=recv_sem.at[sem if r_sem is None else r_sem],
            device_id={"var": v, "samp": s}, device_id_type=pl.DeviceIdType.MESH,
        ).start()

    def got(ref, sem):
        pltpu.make_async_copy(ref, ref, recv_sem.at[sem]).wait()

    def sent(ref, sem):
        pltpu.make_async_copy(ref, ref, send_sem.at[sem]).wait()

    IDS, INV, BETA, SC = 0, 1, 2, 3
    A = 4
    B = A + PASSES
    C = B + PASSES
    SM = C + PASSES
    D = SM + PASSES
    U = D + PASSES
    UQ = U + PASSES

    mk("inputs")
    for c in pulls[:5]:
        c.wait()
    mk("setup")
    for i in range(1, n_loads):
        if i == n_loads // 2:
            for c in pulls[5:]:
                c.start()
        load(i).start()
    ids_all[mv, :, 0:kept] = act_v[...]
    ids_all[mv, :, kept:fit] = adm_v[...]
    index = sidx_v[...]
    scales = jnp.zeros(index.shape, F32)
    for level in range(levels):
        scales = jnp.where(index == level, table_s[level], scales)
    scale_ref[...] = scales
    rlow[...] = cur[...].astype(BF16)
    part[...] = jnp.zeros((ph, width), F32)
    cols = 256

    def screen(i, c):
        for k in range(per_step):
            load(i * per_step + k).wait()
        at = pl.ds(pl.multiple_of(i * step, step), step)
        left = rlow[:, at]
        for j in range(width // cols):
            lane = slice(j * cols, (j + 1) * cols)
            block = []
            for n in range(step // per_group):
                sub = pl.ds(pl.multiple_of(i * step + n * per_group, per_group), per_group)
                scale = scale_ref[pl.ds(i * (step // per_group) + n, 1), lane]
                block.append(x_ref[sub, lane].astype(F32) * scale)
            block = jnp.concatenate(block, axis=0).astype(BF16)
            x_ref[at, lane] = block
            part[:, lane] += dot(left, block)
        return c

    first = (n_steps * 3) // 4
    mk("screen1")
    lax.fori_loop(0, first, screen, 0)
    mk("inv")
    for c in pulls[5:]:
        c.wait()
    for b in range(blocks):
        inv[0, b] = binv_v[b].astype(BF16)
    tri[...] = jnp.where(
        lax.broadcasted_iota(jnp.int32, (fit, fit), 0) < lax.broadcasted_iota(jnp.int32, (fit, fit), 1),
        1.0, 0.0,
    ).astype(BF16)
    mk("barrier")
    pl.semaphore_wait(barrier, N - 1)
    for v in all_var:
        send(ids_all.at[mv], ids_all.at[mv], IDS, v, ms)

    def hand_over():
        send(beta_v, beta_two, BETA, partner, ms)
        send(inv.at[0], inv.at[1], INV, partner, ms)

    other_only(hand_over)
    mk("screen2")
    lax.fori_loop(first, n_steps, screen, 0)
    recv_p[ms] = part[...]

    mk("idswait")
    got(ids_all.at[pl.ds(0, V - 1)], IDS)
    mk("idsproc")
    line = lax.broadcasted_iota(jnp.int32, (V, fit), 0)

    def lines(g):
        return ids_all[g, 0:1, :]

    all_ids = jnp.zeros((V, fit), jnp.int32)
    for g in range(V):
        all_ids = jnp.where(line == g, lines(g), all_ids)
    column = all_ids - mv * width
    held = (column >= 0) & (column < width)
    serial = dot(jnp.where(held, 1.0, 0.0).astype(BF16), tri[...])
    serial = jnp.where(held, serial, -1.0)
    column = jnp.where(held, column, 0)
    eight = lax.broadcasted_iota(jnp.int32, (8, fit), 0)
    turn = lax.broadcasted_iota(jnp.int32, (pad, fit), 0).astype(F32)
    lane_no = lax.broadcasted_iota(jnp.int32, (LANES, pad), 0).astype(F32)
    for n, g in enumerate(order):
        col = column[g:g + 1]
        digits = jnp.where(
            eight == 0, lax.shift_right_logical(col, 7),
            jnp.where(eight == 1, col & 127, jnp.where(eight == 2, 1, 0)),
        ).astype(F32).astype(BF16)
        place = jnp.where(turn == serial[g:g + 1], 1.0, 0.0).astype(BF16)
        found = dot(digits, place, NT)
        here = found[2:3] > 0.5
        at = slice(n * pad, (n + 1) * pad)
        high_t[:, at] = jnp.broadcast_to(jnp.where(here, found[0:1], -1.0), (ph, pad))
        low[:, at] = jnp.where(lane_no == jnp.where(here, found[1:2], -1.0), 1.0, 0.0).astype(BF16)

    mk(None)

    def own_slots():
        mk("own")
        for i in range(G):
            mine = (ids_all[mv if i == 0 else partner][0:1]) - line * width
            marks = jnp.where((mine >= 0) & (mine < width), 1.0, 0.0)
            before = dot(marks.astype(BF16), tri[...])
            position = jnp.sum(marks * before, axis=0, keepdims=True)
            place_v[i] = jnp.where(turn == position, 1.0, 0.0).astype(BF16)
            marks_v[i] = marks
        mk(None)

    def send_gradient(p):
        wide = jnp.concatenate([part[:, t * LANES:(t + 1) * LANES] for t in range(tiles)], axis=0).astype(BF16)
        half = O * G * pad // 2
        for n in range(2):
            at = slice(n * half, (n + 1) * half)
            found = dot(wide, low[:, at])
            which = high_t[:, at]
            out = jnp.zeros((ph, half), F32)
            for t in range(tiles):
                out = jnp.where(which == float(t), found[t * ph:(t + 1) * ph], out)
            out = out.astype(BF16)
            each = G * pad
            for k in range(half // each):
                send_a[p, n * (half // each) + k] = out[:, k * each:(k + 1) * each]
        targets = []
        for k, (v, q) in enumerate(owners):
            for s in samps + [ms]:
                targets.append((v, q, s, k == O - 1 and s is ms))
        for v, q, s, last in targets:
            if not last:
                send(send_a.at[p, q], recv_a.at[p, me], A + p, v, s)
        v, q, s, _ = targets[-1]

        def away():
            send(send_a.at[p, q], recv_a.at[p, me], A + p, v, s)

        other_only(away)

        def stay():
            recv_a[p, me] = send_a[p, q]

        owner_only(stay)

    def wait_sums(p):
        owner_only(lambda: got(recv_s.at[p, pl.ds(0, S * O - 1)], SM + p))
        other_only(lambda: got(recv_s.at[p, pl.ds(0, S * O)], SM + p))

    lane = lax.broadcasted_iota(jnp.int32, (ph, LANES), 1)
    sub = lax.broadcasted_iota(jnp.int32, (ph, LANES), 0)

    def length(p):
        wait_sums(p)
        total = recv_s[p, 0]
        for k in range(1, S * O):
            total = total + recv_s[p, k]
        total = jnp.broadcast_to(total, (ph, LANES))
        cross = jnp.sum(jnp.where(lane == sub, total, 0.0), axis=1, keepdims=True)
        square = jnp.sum(jnp.where(lane == sub + ph, total, 0.0), axis=1, keepdims=True)
        return cross / (square + EPSILON)

    def advance(factor, p, dst):
        for q in range(O):
            at = slice(q * chunk, (q + 1) * chunk)
            dst[:, at] = cur[:, at] - factor * recv_u[p, q].astype(F32)

    def serve(p, factor):
        mk("gotA")
        got(recv_a.at[p, pl.ds(0, N - 1)], A + p)
        mk("serve")
        if p == 0:
            coef[...] = jnp.zeros(coef.shape, F32)
            coef[0, :, 0:kept] = beta_v[...]
            if G > 1:
                got(beta_two, BETA)
                coef[1, :, 0:kept] = beta_two[...]
                got(inv.at[1], INV)
        for i in range(G):
            at = slice(i * pad, (i + 1) * pad)
            stack = []
            for v in range(V):
                val = recv_a[p, v, :, at].astype(F32)
                for s in range(1, S):
                    val = val + recv_a[p, s * V + v, :, at].astype(F32)
                high = val.astype(BF16).astype(F32)
                stack += [high, val - high]
            found = dot(jnp.concatenate(stack, axis=0).astype(BF16), place_v[i])
            slots = jnp.zeros((ph, fit), F32)
            for v in range(V):
                both = found[2 * v * ph:(2 * v + 1) * ph] + found[(2 * v + 1) * ph:(2 * v + 2) * ph]
                slots = slots + marks_v[i, v:v + 1] * both
            slots = slots * inv_root
            if p > 0:
                slots = grad[i] - factor * slots
                coef[i] = coef[i] + factor * direct[p - 1, i].astype(F32)
            grad[i] = slots
            inner = slots - PENALTY * coef[i]
            for b in range(blocks):
                cut = slice(b * bsize, (b + 1) * bsize)
                direct[p, i, :, cut] = joined(dot(split(inner[:, cut]), inv[i, b], NT)).astype(BF16)
            way = direct[p, i].astype(F32)
            spread = jnp.concatenate([way * marks_v[i, v:v + 1] for v in range(V)], axis=0).astype(BF16)
            back = dot(spread, place_v[i], NT).astype(BF16)
            for v in range(V):
                send_b[p, v, :, at] = back[v * ph:(v + 1) * ph]
        mk("sendB")
        for v in all_var:
            send(send_b.at[p, v], recv_b.at[p, my_q], B + p, v, ms)
        if G > 1:
            send(direct.at[p, 1], recv_d.at[p], D + p, partner, ms)
        recv_b[p, my_q] = send_b[p, mv]
        mk(None)

    def reduce(p):
        mk("gotC")
        got(recv_c.at[p, pl.ds(0, V - 1)], C + p)
        mk("sumC")
        val = recv_c[p, 0].astype(F32)
        for v in range(1, V):
            val = val + recv_c[p, v].astype(F32)
        low_u = (val * inv_root).astype(BF16)
        recv_u[p, my_q] = low_u
        for v in all_var:
            send(recv_u.at[p, my_q], recv_u.at[p, my_q], U + p, v, ms, UQ + p * O + my_q)
        mk("sums")
        upd = low_u.astype(F32)
        now = cur[:, pl.ds(pl.multiple_of(my_q * chunk, chunk), chunk)]
        cross = jnp.sum(now * upd, axis=1, keepdims=True)
        square = jnp.sum(upd * upd, axis=1, keepdims=True)
        both = jnp.where(lane == sub, cross, jnp.where(lane == sub + ph, square, 0.0))
        slot = ms * O + my_q
        recv_s[p, slot] = jnp.sum(both, axis=0, keepdims=True)
        for v in all_var:
            for s in samps + [ms]:
                send(recv_s.at[p, slot], recv_s.at[p, slot], SM + p, v, s)
        for s in samps:
            send(recv_s.at[p, slot], recv_s.at[p, slot], SM + p, mv, s)
        mk(None)

    turned = 2 * LANES

    def turn_rows(i, c):
        at = pl.ds(pl.multiple_of(i * turned, turned), turned)
        for j in range(width // turned):
            cut = slice(j * turned, (j + 1) * turned)
            xt_ref[cut, at] = x_ref[at, cut].T
        return c

    owner_only(own_slots)
    factors = []
    for p in range(PASSES):
        mk("gather")
        send_gradient(p)
        mk("mid")
        if p == 0:
            for s in samps:
                send(recv_p.at[ms], recv_p.at[ms], SC, mv, s)
            mk("turn")
            lax.fori_loop(0, rows // turned, turn_rows, 0)
            mk("mid")
        if p == 1:
            got(recv_p.at[pl.ds(0, S - 1)], SC)
            val = recv_p[0]
            for s in range(1, S):
                val = val + recv_p[s]
            scores_out[...] = val * inv_root
        if p > 0:
            factors.append(length(p - 1))
        factor = factors[-1] if p else None
        mk(None)
        owner_only(functools.partial(serve, p, factor))
        mk("adv")
        if p > 0:
            advance(factor, p - 1, cur)
        mk("waitB")
        owner_only(lambda: got(recv_b.at[p, pl.ds(0, O - 1)], B + p))
        other_only(lambda: got(recv_b.at[p, pl.ds(0, O)], B + p))
        mk("spread")
        way = jnp.concatenate([recv_b[p, q] for q in range(O)], axis=1).astype(F32)
        which = high_t[...]
        wide = jnp.concatenate([jnp.where(which == float(t), way, 0.0) for t in range(tiles)], axis=0)
        found = dot(wide.astype(BF16), low[...], NT).astype(BF16)
        for t in range(tiles):
            d_held[:, t * LANES:(t + 1) * LANES] = found[t * ph:(t + 1) * ph]
        mk("upd")

        for k, (v, q) in enumerate(owners):
            if k % join == 0:
                at = pl.ds(pl.multiple_of(lax.div(q, join) * (join * chunk), join * chunk), join * chunk)
                wide = dot(d_held[...], xt_ref[:, at]).astype(BF16)
                first_q = lax.div(q, join) * join
                for i in range(join):
                    send_c[p, first_q + i] = wide[:, i * chunk:(i + 1) * chunk]
            if k < O - 1:
                send(send_c.at[p, q], recv_c.at[p, mv], C + p, v, ms)
            else:

                def away(q=q, v=v):
                    send(send_c.at[p, q], recv_c.at[p, mv], C + p, v, ms)

                other_only(away)

                def stay(q=q):
                    recv_c[p, mv] = send_c[p, q]

                owner_only(stay)
        mk(None)
        owner_only(functools.partial(reduce, p))
        mk("waitU")
        for k, (v, q) in enumerate(reversed(owners)):
            def arrive(q=q):
                got(recv_u.at[p, q], UQ + p * O + q)

            if k == 0:
                other_only(arrive)
            else:
                arrive()
            if p + 1 < PASSES and k % join == join - 1:
                first_q = lax.div(q, join) * join
                at = pl.ds(pl.multiple_of(first_q * chunk, join * chunk), join * chunk)
                new = dot(jnp.concatenate([recv_u[p, first_q + i] for i in range(join)], axis=1), x_ref[at, :])
                if k == join - 1:
                    part[...] = new
                else:
                    part[...] += new

    mk("fin")
    factors.append(length(PASSES - 1))
    factor = factors[-1]
    advance(factor, PASSES - 1, resid_out)

    def own_coef():
        coef_out[...] = coef[0] + factor * direct[PASSES - 1, 0].astype(F32)

    owner_only(own_coef)

    def edge_coef():
        val = jnp.zeros((ph, fit), F32)
        coef[0] = val
        coef[0, :, 0:kept] = beta_v[...]
        val = coef[0]
        for p in range(PASSES):
            got(recv_d.at[p], D + p)
            val = val + factors[p] * recv_d[p].astype(F32)
        coef_out[...] = val

    other_only(edge_coef)
    mk("drain")

    sent(ids_all.at[pl.ds(0, V - 1)], IDS)
    sent(recv_p.at[pl.ds(0, S - 1)], SC)

    def drain_owner():
        for p in range(PASSES):
            sent(recv_a.at[p, pl.ds(0, S * O - 1)], A + p)
            sent(send_b.at[p, pl.ds(0, V - 1)], B + p)
            if O > 1:
                sent(send_c.at[p, pl.ds(0, O - 1)], C + p)
            sent(recv_c.at[p, pl.ds(0, V - 1)], U + p)
            sent(all_rows(p), SM + p)
            if G > 1:
                sent(direct.at[p, 1], D + p)

    def all_rows(p):
        return recv_s.at[p, pl.ds(0, N - 1)]

    owner_only(drain_owner)

    def drain_other():
        sent(beta_v, BETA)
        sent(inv.at[0], INV)
        for p in range(PASSES):
            sent(recv_a.at[p, pl.ds(0, S * O)], A + p)
            sent(send_c.at[p], C + p)

    other_only(drain_other)


def on_device(geno, scale_index, scale_table, residual, beta_active, block_inverse, active_ids, admit_ids):
    V, S = lax.axis_size("var"), lax.axis_size("samp")
    N = V * S
    O, G = owners_of(V)
    rows, width = geno.shape
    ph = residual.shape[0]
    fit = active_ids.shape[0] + admit_ids.shape[0]
    pad = LANES * pl.cdiv(2 * fit // V, LANES)
    chunk = rows // O
    vmem = pl.BlockSpec(memory_space=pltpu.VMEM)
    hbm = pl.BlockSpec(memory_space=pl.ANY)
    n_send = 4 + 6 * PASSES
    n_recv = n_send + PASSES * O
    per_group = rows // scale_index.shape[0]
    out = pl.pallas_call(
        functools.partial(kernel, V, S, pad),
        out_shape=(pltpu.VMEM((ph, width), F32), pltpu.VMEM((ph, fit), F32), pltpu.VMEM((ph, rows), F32)),
        in_specs=[hbm] * 8,
        out_specs=(vmem, vmem, vmem),
        scratch_shapes=[
            pltpu.VMEM((rows, width), BF16),
            pltpu.VMEM((width, rows), BF16),
            pltpu.VMEM(scale_index.shape, jnp.int32),
            pltpu.SMEM(scale_table.shape, F32),
            pltpu.VMEM((ph, rows), F32),
            pltpu.VMEM(beta_active.shape, F32),
            pltpu.VMEM(block_inverse.shape, F32),
            pltpu.VMEM((1, active_ids.shape[0]), jnp.int32),
            pltpu.VMEM((1, admit_ids.shape[0]), jnp.int32),
            pltpu.VMEM(scale_index.shape, F32),
            pltpu.VMEM((ph, rows), BF16),
            pltpu.VMEM((ph, width), F32),
            pltpu.VMEM((LANES, V * pad), BF16),
            pltpu.VMEM((ph, V * pad), F32),
            pltpu.VMEM((G, V, fit), F32),
            pltpu.VMEM((G, pad, fit), BF16),
            pltpu.VMEM((fit, fit), BF16),
            pltpu.VMEM((G,) + block_inverse.shape, BF16),
            pltpu.VMEM(beta_active.shape, F32),
            pltpu.VMEM((V, 1, fit), jnp.int32),
            pltpu.VMEM((ph, width), BF16),
            pltpu.VMEM((G, ph, fit), F32),
            pltpu.VMEM((G, ph, fit), F32),
            pltpu.VMEM((PASSES, G, ph, fit), BF16),
            pltpu.VMEM((PASSES, O, ph, G * pad), BF16),
            pltpu.VMEM((PASSES, N, ph, G * pad), BF16),
            pltpu.VMEM((PASSES, V, ph, G * pad), BF16),
            pltpu.VMEM((PASSES, O, ph, G * pad), BF16),
            pltpu.VMEM((PASSES, O, ph, chunk), BF16),
            pltpu.VMEM((PASSES, V, ph, chunk), BF16),
            pltpu.VMEM((PASSES, O, ph, chunk), BF16),
            pltpu.VMEM((S, ph, width), F32),
            pltpu.VMEM((PASSES, N, 1, LANES), F32),
            pltpu.VMEM((PASSES, ph, fit), BF16),
            pltpu.SemaphoreType.DMA((rows // (2 * per_group),)),
            pltpu.SemaphoreType.DMA((7,)),
            pltpu.SemaphoreType.DMA((n_send,)),
            pltpu.SemaphoreType.DMA((n_recv,)),
        ],
        compiler_params=pltpu.CompilerParams(
            collective_id=0, has_side_effects=True, vmem_limit_bytes=60 * 1024 * 1024
        ),
    )(geno, scale_index, scale_table, residual, beta_active, block_inverse, active_ids[None], admit_ids[None])

    def hand_out(*refs):
        half = len(refs) // 2
        for a, b in zip(refs[:half], refs[half:]):
            b[...] = a[...]

    return pl.pallas_call(
        hand_out, out_shape=tuple(jax.ShapeDtypeStruct(o.shape, o.dtype) for o in out),
        in_specs=[vmem] * 3, out_specs=(vmem,) * 3,
        compiler_params=pltpu.CompilerParams(vmem_limit_bytes=1024 * 1024),
    )(*out)


def solution(mesh):
    placed = (
        P("samp", "var"), P("samp", "var"), P(), P(None, "samp"), P(None, "var"),
        P("var", None, None), P("var"), P("var"),
    )
    return jax.shard_map(
        on_device, mesh=mesh, in_specs=placed,
        out_specs=(P(None, "var"), P(None, "var"), P(None, "samp")), check_vma=False,
    )
```

```python
import functools
import math

import jax
import jax.numpy as jnp
from jax import lax
from jax.experimental import pallas as pl
from jax.experimental.pallas import tpu as pltpu
from jax.sharding import PartitionSpec as P

PASSES = 3
PENALTY = 0.5
EPSILON = 1e-06
LANES = 128
F32 = jnp.float32
BF16 = jnp.bfloat16
NN = (((1,), (0,)), ((), ()))
NT = (((1,), (1,)), ((), ()))


def dot(a, b, dims=NN):
    return lax.dot_general(a, b, dims, preferred_element_type=F32)


def split(x):
    high = x.astype(BF16).astype(F32)
    return jnp.concatenate([high, x - high], axis=0).astype(BF16)


def joined(x):
    half = x.shape[0] // 2
    return x[:half] + x[half:]


def kernel(
    V, S, pad,
    geno, sidx, table, resid, beta, binv, active, admit,
    scores_out, coef_out, resid_out,
    x_ref, xt_ref, sidx_v, table_s, cur, beta_v, binv_v, act_v, adm_v,
    scale_ref, rlow, part, low, high_t, marks_v, place_v, tri, inv, beta_two, ids_all, blank,
    d_held, coef, grad, direct,
    send_a, recv_a, send_b, recv_b, send_c, recv_c, recv_u, recv_p, recv_s, recv_d,
    load_sem, in_sem, send_sem, recv_sem,
):
    cur_scope = [None]

    def mk(name):
        pass

    N = V * S
    H, O = V // 8, V // 4
    rows, width = x_ref.shape
    groups = sidx_v.shape[0]
    per_group = rows // groups
    levels = table_s.shape[0]
    ph = cur.shape[0]
    kept = act_v.shape[1]
    fit = kept + adm_v.shape[1]
    blocks, bsize = binv_v.shape[0], binv_v.shape[1]
    chunk = rows // O
    tiles = width // LANES
    piece = 2 * per_group
    n_loads = rows // piece
    per_step = 2 if n_loads % 2 == 0 else 1
    step = per_step * piece
    n_steps = rows // step
    inv_root = 1.0 / math.sqrt(rows * S)
    mv, ms = lax.axis_index("var"), lax.axis_index("samp")
    me = ms * V + mv

    mk("greet")
    barrier = pltpu.get_barrier_semaphore()

    samps = [lax.rem(ms + d, S) for d in range(1, S)] + [ms]
    if S == 4:
        samps = [3 - ms] + [ms + d - 2 * d * lax.rem(lax.div(ms, d), 2) for d in (2, 1)] + [ms]
    others = [lax.rem(mv + d, V) for d in range(V - 1, -1, -1)]
    for s in samps:
        for v in others[:-1] if s is ms else others:
            pl.semaphore_signal(
                barrier, inc=1, device_id={"var": v, "samp": s}, device_id_type=pl.DeviceIdType.MESH
            )
    mk("start")

    def load(i):
        at = pl.ds(pl.multiple_of(i * piece, piece), piece)
        return pltpu.make_async_copy(geno.at[at], x_ref.at[at], load_sem.at[i])

    small = [(table, table_s), (sidx, sidx_v), (resid, cur), (active, act_v), (admit, adm_v), (beta, beta_v), (binv, binv_v)]
    pulls = [pltpu.make_async_copy(a, b, in_sem.at[i]) for i, (a, b) in enumerate(small)]
    for c in pulls[:5]:
        c.start()
    load(0).start()
    load(1).start()

    h, z, c0 = lax.div(mv, 8), lax.rem(lax.div(mv, 2), 4), lax.rem(mv, 2)
    side = lax.div(z, 2)
    hs = [lax.rem(h + d, H) for d in range(1, H)] + [h]
    halves = [(hh, ss) for hh in hs for ss in (1 - side, side)]
    owners = [(8 * hh + 2 * (1 + ss) + 1, 2 * hh + ss) for hh, ss in halves]
    is_owner = jnp.logical_and(z == 1 + side, c0 == 1)
    my_q = 2 * h + side
    my_g = 8 * h + 4 * side + lax.rem(ms, 4)
    serves = jnp.logical_and(is_owner, ms < 4)
    own_turn = ms == 2 * lax.rem(z, 2) + c0
    keeps = jnp.logical_and(is_owner, own_turn)
    gives = jnp.logical_and(own_turn, jnp.logical_not(is_owner))
    taker = 8 * h + 2 * (1 + side) + 1
    z0 = z + side * (3 - 2 * z)
    zs = [side * 3 + (1 - 2 * side) * k for k in (3, 2, 1 - z0, z0)]
    all_var = [8 * hh + 2 * zz + cc for hh in hs for zz in zs for cc in (1 - c0, c0)][:-1]
    samps = samps[:-1]

    def owner_only(fn):
        pl.when(is_owner)(fn)

    def other_only(fn):
        pl.when(jnp.logical_not(is_owner))(fn)

    def unless(cond, fn):
        pl.when(jnp.logical_not(cond))(fn)

    def send(src, dst, sem, v, s, r_sem=None):
        pltpu.make_async_remote_copy(
            src_ref=src, dst_ref=dst, send_sem=send_sem.at[sem],
            recv_sem=recv_sem.at[sem if r_sem is None else r_sem],
            device_id={"var": v, "samp": s}, device_id_type=pl.DeviceIdType.MESH,
        ).start()

    def got(ref, sem):
        pltpu.make_async_copy(ref, ref, recv_sem.at[sem]).wait()

    def sent(ref, sem):
        pltpu.make_async_copy(ref, ref, send_sem.at[sem]).wait()

    IDS, INV, BETA, SC = 0, 1, 2, 3
    A = 4
    B = A + PASSES
    C = B + PASSES
    SM = C + PASSES
    D = SM + PASSES
    U = D + PASSES
    UQ = U + PASSES

    tri[...] = jnp.where(
        lax.broadcasted_iota(jnp.int32, (fit, fit), 0) < lax.broadcasted_iota(jnp.int32, (fit, fit), 1),
        1.0, 0.0,
    ).astype(BF16)
    part[...] = jnp.zeros((ph, width), F32)
    mk("inputs")
    for c in pulls[:5]:
        c.wait()
    mk("setup")
    for i in range(2, n_loads):
        if i == n_loads // 2:
            for c in pulls[5:]:
                c.start()
        load(i).start()
    ids_all[mv, :, 0:kept] = act_v[...]
    ids_all[mv, :, kept:fit] = adm_v[...]
    index = sidx_v[...]
    scales = jnp.zeros(index.shape, F32)
    for level in range(levels):
        scales = jnp.where(index == level, table_s[level], scales)
    scale_ref[...] = scales
    rlow[...] = cur[...].astype(BF16)
    cols = 256

    def screen(i, c):
        for k in range(per_step):
            load(i * per_step + k).wait()
        at = pl.ds(pl.multiple_of(i * step, step), step)
        left = rlow[:, at]
        for j in range(width // cols):
            lane = slice(j * cols, (j + 1) * cols)
            block = []
            for n in range(step // per_group):
                sub = pl.ds(pl.multiple_of(i * step + n * per_group, per_group), per_group)
                scale = scale_ref[pl.ds(i * (step // per_group) + n, 1), lane]
                block.append(x_ref[sub, lane].astype(F32) * scale)
            block = jnp.concatenate(block, axis=0).astype(BF16)
            x_ref[at, lane] = block
            part[:, lane] += dot(left, block)
        return c

    first = pl.cdiv(n_steps, 4)
    mk("screen1")
    lax.fori_loop(0, first, screen, 0)
    mk("barrier")
    pl.semaphore_wait(barrier, N - 1)
    for v in all_var:
        send(ids_all.at[mv], ids_all.at[mv], IDS, v, ms)

    mk("screen2")
    lax.fori_loop(first, n_steps, screen, 0)
    recv_p[ms] = part[...]
    mk("inv")
    for c in pulls[5:]:
        c.wait()
    for b in range(blocks):
        inv[0, b] = binv_v[b].astype(BF16)

    def hand_over():
        send(beta_v, beta_two, BETA, taker, ms)
        send(inv.at[0], inv.at[1], INV, taker, ms)

    pl.when(gives)(hand_over)

    def keep():
        beta_two[...] = beta_v[...]
        inv[1] = inv[0]

    pl.when(keeps)(keep)
    mk("idswait")
    got(ids_all.at[pl.ds(0, V - 1)], IDS)
    mk("idsproc")
    line = lax.broadcasted_iota(jnp.int32, (V, fit), 0)

    def lines(g):
        return ids_all[g, 0:1, :]

    all_ids = jnp.zeros((V, fit), jnp.int32)
    for g in range(V):
        all_ids = jnp.where(line == g, lines(g), all_ids)
    column = all_ids - mv * width
    held = (column >= 0) & (column < width)
    serial = dot(jnp.where(held, 1.0, 0.0).astype(BF16), tri[...])
    serial = jnp.where(held, serial, -1.0)
    column = jnp.where(held, column, 0)
    eight = lax.broadcasted_iota(jnp.int32, (8, fit), 0)
    turn = lax.broadcasted_iota(jnp.int32, (pad, fit), 0).astype(F32)
    lane_no = lax.broadcasted_iota(jnp.int32, (LANES, pad), 0).astype(F32)
    for g in range(V):
        col = column[g:g + 1]
        digits = jnp.where(
            eight == 0, lax.shift_right_logical(col, 7),
            jnp.where(eight == 1, col & 127, jnp.where(eight == 2, 1, 0)),
        ).astype(F32).astype(BF16)
        place = jnp.where(turn == serial[g:g + 1], 1.0, 0.0).astype(BF16)
        found = dot(digits, place, NT)
        here = found[2:3] > 0.5
        at = slice(g * pad, (g + 1) * pad)
        high_t[:, at] = jnp.broadcast_to(jnp.where(here, found[0:1], -1.0), (ph, pad))
        low[:, at] = jnp.where(lane_no == jnp.where(here, found[1:2], -1.0), 1.0, 0.0).astype(BF16)

    mk(None)

    def own_slots():
        mk("own")
        mine = ids_all[my_g][0:1] - line * width
        marks = jnp.where((mine >= 0) & (mine < width), 1.0, 0.0)
        before = dot(marks.astype(BF16), tri[...])
        position = jnp.sum(marks * before, axis=0, keepdims=True)
        place_v[...] = jnp.where(turn == position, 1.0, 0.0).astype(BF16)
        marks_v[...] = marks
        mk(None)

    def send_gradient(p):
        wide = jnp.concatenate([part[:, t * LANES:(t + 1) * LANES] for t in range(tiles)], axis=0).astype(BF16)
        for n, (hh, ss) in enumerate(halves):
            base = 8 * hh + 4 * ss
            at = pl.ds(pl.multiple_of(base * pad, 4 * pad), 4 * pad)
            found = dot(wide, low[:, at])
            which = high_t[:, at]
            out = jnp.zeros((ph, 4 * pad), F32)
            for t in range(tiles):
                out = jnp.where(which == float(t), found[t * ph:(t + 1) * ph], out)
            out = out.astype(BF16)
            for k in range(4):
                send_a[p, base + k] = out[:, k * pad:(k + 1) * pad]
            v = 8 * hh + 2 * (1 + ss) + 1
            last = n == len(halves) - 1
            turns = [lax.rem(ms + d, 4) for d in (2, 3, 1)]
            for r in turns if last else turns + [lax.rem(ms, 4)]:
                send(send_a.at[p, base + r], recv_a.at[p, me], A + p, v, r)

        def away():
            send(send_a.at[p, my_g], recv_a.at[p, me], A + p, taker, lax.rem(ms, 4))

        unless(serves, away)

        def stay():
            recv_a[p, me] = send_a[p, my_g]

        pl.when(serves)(stay)

    def wait_sums(p):
        owner_only(lambda: got(recv_s.at[p, pl.ds(0, S * O - 1)], SM + p))
        other_only(lambda: got(recv_s.at[p, pl.ds(0, S * O)], SM + p))

    lane = lax.broadcasted_iota(jnp.int32, (ph, LANES), 1)
    sub = lax.broadcasted_iota(jnp.int32, (ph, LANES), 0)

    def length(p):
        wait_sums(p)
        total = recv_s[p, 0]
        for k in range(1, S * O):
            total = total + recv_s[p, k]
        total = jnp.broadcast_to(total, (ph, LANES))
        cross = jnp.sum(jnp.where(lane == sub, total, 0.0), axis=1, keepdims=True)
        square = jnp.sum(jnp.where(lane == sub + ph, total, 0.0), axis=1, keepdims=True)
        return cross / (square + EPSILON)

    def advance(factor, p, dst):
        for q in range(O):
            at = slice(q * chunk, (q + 1) * chunk)
            dst[:, at] = cur[:, at] - factor * recv_u[p, q].astype(F32)

    def serve(p, factor):
        mk("gotA")
        got(recv_a.at[p, pl.ds(0, N - 1)], A + p)
        mk("serve")
        if p == 0:
            def take():
                got(beta_two, BETA)
                got(inv.at[1], INV)

            unless(keeps, take)
            coef[...] = jnp.zeros(coef.shape, F32)
            coef[:, 0:kept] = beta_two[...]
        stack = []
        for v in range(V):
            val = recv_a[p, v].astype(F32)
            for s in range(1, S):
                val = val + recv_a[p, s * V + v].astype(F32)
            high = val.astype(BF16).astype(F32)
            stack += [high, val - high]
        found = dot(jnp.concatenate(stack, axis=0).astype(BF16), place_v[...])
        slots = jnp.zeros((ph, fit), F32)
        for v in range(V):
            both = found[2 * v * ph:(2 * v + 1) * ph] + found[(2 * v + 1) * ph:(2 * v + 2) * ph]
            slots = slots + marks_v[v:v + 1] * both
        slots = slots * inv_root
        if p > 0:
            slots = grad[...] - factor * slots
            coef[...] = coef[...] + factor * direct[p - 1].astype(F32)
        grad[...] = slots
        inner = slots - PENALTY * coef[...]
        ways = []
        for b in range(blocks):
            cut = slice(b * bsize, (b + 1) * bsize)
            ways.append(joined(dot(split(inner[:, cut]), inv[1, b], NT)).astype(BF16))
        way = jnp.concatenate(ways, axis=1)
        direct[p] = way
        way = way.astype(F32)
        spread = jnp.concatenate([way * marks_v[v:v + 1] for v in range(V)], axis=0).astype(BF16)
        back = dot(spread, place_v[...], NT).astype(BF16)
        for v in range(V):
            send_b[p, v] = back[v * ph:(v + 1) * ph]
        mk("sendB")
        for s in samps + [ms]:
            for v in all_var:
                send(send_b.at[p, v], recv_b.at[p, my_g], B + p, v, s)
        for s in samps:
            send(send_b.at[p, mv], recv_b.at[p, my_g], B + p, mv, s)
        recv_b[p, my_g] = send_b[p, mv]
        for s in samps:
            send(direct.at[p], recv_d.at[p], D + p, my_g, s)

        def away():
            send(direct.at[p], recv_d.at[p], D + p, my_g, ms)

        unless(keeps, away)

        def stay():
            recv_d[p] = direct[p]

        pl.when(keeps)(stay)
        mk(None)

    def reduce(p):
        mk("gotC")
        got(recv_c.at[p, pl.ds(0, V - 1)], C + p)
        mk("sumC")
        val = recv_c[p, 0].astype(F32)
        for v in range(1, V):
            val = val + recv_c[p, v].astype(F32)
        low_u = (val * inv_root).astype(BF16)
        recv_u[p, my_q] = low_u

        def tell_update():
            for v in all_var:
                send(recv_u.at[p, my_q], recv_u.at[p, my_q], U + p, v, ms, UQ + p * O + my_q)

        def tell_sums():
            upd = low_u.astype(F32)
            now = cur[:, pl.ds(pl.multiple_of(my_q * chunk, chunk), chunk)]
            cross = jnp.sum(now * upd, axis=1, keepdims=True)
            square = jnp.sum(upd * upd, axis=1, keepdims=True)
            both = jnp.where(lane == sub, cross, jnp.where(lane == sub + ph, square, 0.0))
            slot = ms * O + my_q
            recv_s[p, slot] = jnp.sum(both, axis=0, keepdims=True)
            for s in samps + [ms]:
                for v in all_var:
                    send(recv_s.at[p, slot], recv_s.at[p, slot], SM + p, v, s)
            for s in samps:
                send(recv_s.at[p, slot], recv_s.at[p, slot], SM + p, mv, s)

        if p + 1 < PASSES:
            tell_update()
            tell_sums()
        else:
            tell_sums()
            tell_update()
        mk(None)

    turned = 2 * LANES

    def turn_rows(i, c):
        at = pl.ds(pl.multiple_of(i * turned, turned), turned)
        for j in range(width // turned):
            cut = slice(j * turned, (j + 1) * turned)
            xt_ref[cut, at] = x_ref[at, cut].T
        return c

    pl.when(serves)(own_slots)
    factors = []
    for p in range(PASSES):
        mk("gather")
        send_gradient(p)
        mk("mid")
        if p == 0:
            for s in samps:
                send(recv_p.at[ms], recv_p.at[ms], SC, mv, s)
            mk("turn")
            lax.fori_loop(0, rows // turned, turn_rows, 0)
            mk("mid")
        if p == 1:
            got(recv_p.at[pl.ds(0, S - 1)], SC)
            val = recv_p[0]
            for s in range(1, S):
                val = val + recv_p[s]
            scores_out[...] = val * inv_root
        if p > 0:
            factors.append(length(p - 1))
        factor = factors[-1] if p else None
        mk(None)
        pl.when(serves)(functools.partial(serve, p, factor))
        mk("adv")
        if p > 0:
            advance(factor, p - 1, cur)
        mk("waitB")
        pl.when(serves)(lambda: got(recv_b.at[p, pl.ds(0, V - 1)], B + p))
        unless(serves, lambda: got(recv_b.at[p], B + p))
        mk("spread")
        way = jnp.concatenate([recv_b[p, g] for g in range(V)], axis=1).astype(F32)
        which = high_t[...]
        wide = jnp.concatenate([jnp.where(which == float(t), way, 0.0) for t in range(tiles)], axis=0)
        found = dot(wide.astype(BF16), low[...], NT).astype(BF16)
        for t in range(tiles):
            d_held[:, t * LANES:(t + 1) * LANES] = found[t * ph:(t + 1) * ph]
        mk("upd")

        for k, (v, q) in enumerate(owners):
            at = pl.ds(pl.multiple_of(q * chunk, chunk), chunk)
            send_c[p, q] = dot(d_held[...], xt_ref[:, at]).astype(BF16)
            if k < O - 1:
                send(send_c.at[p, q], recv_c.at[p, mv], C + p, v, ms)
            else:
                def away(q=q, v=v):
                    send(send_c.at[p, q], recv_c.at[p, mv], C + p, v, ms)

                other_only(away)

                def stay(q=q):
                    recv_c[p, mv] = send_c[p, q]

                owner_only(stay)
        mk(None)
        owner_only(functools.partial(reduce, p))
        mk("waitU")
        for k, (v, q) in enumerate(reversed(owners)):
            def arrive(q=q):
                got(recv_u.at[p, q], UQ + p * O + q)

            if k == 0:
                other_only(arrive)
            else:
                arrive()
            if p + 1 < PASSES:
                at = pl.ds(pl.multiple_of(q * chunk, chunk), chunk)
                new = dot(recv_u[p, q], x_ref[at, :])
                if k == 0:
                    part[...] = new
                else:
                    part[...] += new

    mk("fin")
    factors.append(length(PASSES - 1))
    factor = factors[-1]
    advance(factor, PASSES - 1, resid_out)

    coef_out[...] = jnp.zeros((ph, fit), F32)
    coef_out[:, 0:kept] = beta_v[...]
    val = coef_out[...]
    for p in range(PASSES):
        unless(keeps, functools.partial(lambda p: got(recv_d.at[p], D + p), p))
        val = val + factors[p] * recv_d[p].astype(F32)
    coef_out[...] = val
    mk("drain")

    sent(ids_all.at[pl.ds(0, V - 1)], IDS)
    sent(recv_p.at[pl.ds(0, S - 1)], SC)

    def drain_a(p):
        pl.when(serves)(lambda: sent(recv_a.at[p, pl.ds(0, V - 1)], A + p))
        unless(serves, lambda: sent(recv_a.at[p, pl.ds(0, V)], A + p))

    def drain_serve():
        for p in range(PASSES):
            sent(recv_a.at[p, pl.ds(0, N - 1)], B + p)
            pl.when(keeps)(functools.partial(lambda p: sent(blank.at[pl.ds(0, S - 1)], D + p), p))
            unless(keeps, functools.partial(lambda p: sent(blank, D + p), p))

    def drain_owner():
        for p in range(PASSES):
            sent(send_c.at[p, pl.ds(0, O - 1)], C + p)
            sent(recv_c.at[p, pl.ds(0, V - 1)], U + p)
            sent(recv_s.at[p, pl.ds(0, N - 1)], SM + p)

    def drain_other():
        for p in range(PASSES):
            sent(send_c.at[p], C + p)

    def drain_gives():
        sent(beta_v, BETA)
        sent(inv.at[0], INV)

    for p in range(PASSES):
        drain_a(p)
    pl.when(serves)(drain_serve)
    owner_only(drain_owner)
    pl.when(gives)(drain_gives)
    other_only(drain_other)


def on_device(geno, scale_index, scale_table, residual, beta_active, block_inverse, active_ids, admit_ids):
    V, S = lax.axis_size("var"), lax.axis_size("samp")
    N = V * S
    O = V // 4
    assert V % 8 == 0 and S >= 4
    rows, width = geno.shape
    ph = residual.shape[0]
    fit = active_ids.shape[0] + admit_ids.shape[0]
    pad = LANES * pl.cdiv(2 * fit // V, LANES)
    chunk = rows // O
    vmem = pl.BlockSpec(memory_space=pltpu.VMEM)
    hbm = pl.BlockSpec(memory_space=pl.ANY)
    n_send = 4 + 6 * PASSES
    n_recv = n_send + PASSES * O
    per_group = rows // scale_index.shape[0]
    out = pl.pallas_call(
        functools.partial(kernel, V, S, pad),
        out_shape=(pltpu.VMEM((ph, width), F32), pltpu.VMEM((ph, fit), F32), pltpu.VMEM((ph, rows), F32)),
        in_specs=[hbm] * 8,
        out_specs=(vmem, vmem, vmem),
        scratch_shapes=[
            pltpu.VMEM((rows, width), BF16),
            pltpu.VMEM((width, rows), BF16),
            pltpu.VMEM(scale_index.shape, jnp.int32),
            pltpu.SMEM(scale_table.shape, F32),
            pltpu.VMEM((ph, rows), F32),
            pltpu.VMEM(beta_active.shape, F32),
            pltpu.VMEM(block_inverse.shape, F32),
            pltpu.VMEM((1, active_ids.shape[0]), jnp.int32),
            pltpu.VMEM((1, admit_ids.shape[0]), jnp.int32),
            pltpu.VMEM(scale_index.shape, F32),
            pltpu.VMEM((ph, rows), BF16),
            pltpu.VMEM((ph, width), F32),
            pltpu.VMEM((LANES, V * pad), BF16),
            pltpu.VMEM((ph, V * pad), F32),
            pltpu.VMEM((V, fit), F32),
            pltpu.VMEM((pad, fit), BF16),
            pltpu.VMEM((fit, fit), BF16),
            pltpu.VMEM((2,) + block_inverse.shape, BF16),
            pltpu.VMEM(beta_active.shape, F32),
            pltpu.VMEM((V, 1, fit), jnp.int32),
            pltpu.VMEM((S, ph, fit), BF16),
            pltpu.VMEM((ph, width), BF16),
            pltpu.VMEM((ph, fit), F32),
            pltpu.VMEM((ph, fit), F32),
            pltpu.VMEM((PASSES, ph, fit), BF16),
            pltpu.VMEM((PASSES, V, ph, pad), BF16),
            pltpu.VMEM((PASSES, N, ph, pad), BF16),
            pltpu.VMEM((PASSES, V, ph, pad), BF16),
            pltpu.VMEM((PASSES, V, ph, pad), BF16),
            pltpu.VMEM((PASSES, O, ph, chunk), BF16),
            pltpu.VMEM((PASSES, V, ph, chunk), BF16),
            pltpu.VMEM((PASSES, O, ph, chunk), BF16),
            pltpu.VMEM((S, ph, width), F32),
            pltpu.VMEM((PASSES, N, 1, LANES), F32),
            pltpu.VMEM((PASSES, ph, fit), BF16),
            pltpu.SemaphoreType.DMA((rows // (2 * per_group),)),
            pltpu.SemaphoreType.DMA((7,)),
            pltpu.SemaphoreType.DMA((n_send,)),
            pltpu.SemaphoreType.DMA((n_recv,)),
        ],
        compiler_params=pltpu.CompilerParams(
            collective_id=0, has_side_effects=True, vmem_limit_bytes=60 * 1024 * 1024
        ),
    )(geno, scale_index, scale_table, residual, beta_active, block_inverse, active_ids[None], admit_ids[None])

    def hand_out(*refs):
        half = len(refs) // 2
        for a, b in zip(refs[:half], refs[half:]):
            b[...] = a[...]

    return pl.pallas_call(
        hand_out, out_shape=tuple(jax.ShapeDtypeStruct(o.shape, o.dtype) for o in out),
        in_specs=[vmem] * 3, out_specs=(vmem,) * 3,
        compiler_params=pltpu.CompilerParams(vmem_limit_bytes=1024 * 1024),
    )(*out)


def solution(mesh):
    placed = (
        P("samp", "var"), P("samp", "var"), P(), P(None, "samp"), P(None, "var"),
        P("var", None, None), P("var"), P("var"),
    )
    return jax.shard_map(
        on_device, mesh=mesh, in_specs=placed,
        out_specs=(P(None, "var"), P(None, "var"), P(None, "samp")), check_vma=False,
    )
```

```python
import functools
import math

import jax
import jax.numpy as jnp
from jax import lax
from jax.experimental import pallas as pl
from jax.experimental.pallas import tpu as pltpu
from jax.sharding import PartitionSpec as P

PASSES = 3
PENALTY = 0.5
EPSILON = 1e-06
LANES = 128
F32 = jnp.float32
BF16 = jnp.bfloat16
NN = (((1,), (0,)), ((), ()))
NT = (((1,), (1,)), ((), ()))


def dot(a, b, dims=NN):
    return lax.dot_general(a, b, dims, preferred_element_type=F32)


def split(x):
    high = x.astype(BF16).astype(F32)
    return jnp.concatenate([high, x - high], axis=0).astype(BF16)


def joined(x):
    half = x.shape[0] // 2
    return x[:half] + x[half:]


def kernel(
    V, S, pad,
    geno, sidx, table, resid, beta, binv, active, admit,
    scores_out, coef_out, resid_out,
    x_ref, xt_ref, sidx_v, table_s, cur, beta_v, binv_v, act_v, adm_v,
    scale_ref, rlow, part, low, high_t, marks_v, place_v, tri, inv, beta_two, ids_all, blank,
    d_held, coef, grad, direct,
    send_a, recv_a, send_b, recv_b, send_c, recv_c, recv_u, recv_p, recv_s, recv_d,
    load_sem, in_sem, send_sem, recv_sem,
):
    cur_scope = [None]

    def mk(name):
        pass

    N = V * S
    H, O = V // 8, V // 4
    rows, width = x_ref.shape
    groups = sidx_v.shape[0]
    per_group = rows // groups
    levels = table_s.shape[0]
    ph = cur.shape[0]
    kept = act_v.shape[1]
    fit = kept + adm_v.shape[1]
    blocks, bsize = binv_v.shape[0], binv_v.shape[1]
    chunk = rows // O
    tiles = width // LANES
    piece = 2 * per_group
    n_loads = rows // piece
    inv_root = 1.0 / math.sqrt(rows * S)
    mv, ms = lax.axis_index("var"), lax.axis_index("samp")
    me = ms * V + mv

    mk("greet")
    barrier = pltpu.get_barrier_semaphore()

    samps = [lax.rem(ms + d, S) for d in range(1, S)]
    if S == 4:
        samps = [3 - ms] + [ms + d - 2 * d * lax.rem(lax.div(ms, d), 2) for d in (2, 1)]

    h, z, c0 = lax.div(mv, 8), lax.rem(lax.div(mv, 2), 4), lax.rem(mv, 2)
    side = lax.div(z, 2)
    hs = [lax.rem(h + d, H) for d in range(1, H)] + [h]
    halves = [(hh, ss) for hh in hs for ss in (1 - side, side)]
    owners = [(8 * hh + 2 * (1 + ss) + 1, 2 * hh + ss) for hh, ss in halves]
    is_owner = jnp.logical_and(z == 1 + side, c0 == 1)
    my_q = 2 * h + side
    my_g = 8 * h + 4 * side + lax.rem(ms, 4)
    serves = jnp.logical_and(is_owner, ms < 4)
    own_turn = ms == 2 * lax.rem(z, 2) + c0
    keeps = jnp.logical_and(is_owner, own_turn)
    gives = jnp.logical_and(own_turn, jnp.logical_not(is_owner))
    taker = 8 * h + 2 * (1 + side) + 1
    z0 = z + side * (3 - 2 * z)
    zs = [side * 3 + (1 - 2 * side) * k for k in (3, 2, 1 - z0, z0)]
    all_var = [8 * hh + 2 * zz + cc for hh in hs for zz in zs for cc in (1 - c0, c0)][:-1]

    def hello(v, s):
        pl.semaphore_signal(
            barrier, inc=1, device_id={"var": v, "samp": s}, device_id_type=pl.DeviceIdType.MESH
        )

    for v in all_var:
        hello(v, ms)
    for s in samps:
        hello(mv, s)

    def greet_all():
        for s in samps:
            for v in all_var:
                hello(v, s)

    pl.when(is_owner)(greet_all)

    def greet_owners():
        for s in samps:
            for v, _ in owners:
                hello(v, s)

    pl.when(jnp.logical_not(is_owner))(greet_owners)
    mk("start")

    def load(i):
        at = pl.ds(pl.multiple_of(i * piece, piece), piece)
        return pltpu.make_async_copy(geno.at[at], x_ref.at[at], load_sem.at[i])

    small = [(table, table_s), (sidx, sidx_v), (resid, cur), (active, act_v), (admit, adm_v), (beta, beta_v), (binv, binv_v)]
    pulls = [pltpu.make_async_copy(a, b, in_sem.at[i]) for i, (a, b) in enumerate(small)]
    for c in pulls[:5]:
        c.start()
    load(0).start()
    for c in pulls[5:]:
        c.start()


    def owner_only(fn):
        pl.when(is_owner)(fn)

    def other_only(fn):
        pl.when(jnp.logical_not(is_owner))(fn)

    def unless(cond, fn):
        pl.when(jnp.logical_not(cond))(fn)

    def send(src, dst, sem, v, s, r_sem=None):
        pltpu.make_async_remote_copy(
            src_ref=src, dst_ref=dst, send_sem=send_sem.at[sem],
            recv_sem=recv_sem.at[sem if r_sem is None else r_sem],
            device_id={"var": v, "samp": s}, device_id_type=pl.DeviceIdType.MESH,
        ).start()

    def got(ref, sem):
        pltpu.make_async_copy(ref, ref, recv_sem.at[sem]).wait()

    def sent(ref, sem):
        pltpu.make_async_copy(ref, ref, send_sem.at[sem]).wait()

    IDS, INV, BETA, SC = 0, 1, 2, 3
    A = 4
    B = A + PASSES
    C = B + PASSES
    SM = C + PASSES
    D = SM + PASSES
    U = D + PASSES
    UQ = U + PASSES
    IQ = UQ + PASSES * O

    tri[...] = jnp.where(
        lax.broadcasted_iota(jnp.int32, (fit, fit), 0) < lax.broadcasted_iota(jnp.int32, (fit, fit), 1),
        1.0, 0.0,
    ).astype(BF16)
    part[...] = jnp.zeros((ph, width), F32)
    mk("inputs")
    for c in pulls[:5]:
        c.wait()
    mk("setup")
    for i in range(1, n_loads):
        load(i).start()
    ids_all[mv, :, 0:kept] = act_v[...]
    ids_all[mv, :, kept:fit] = adm_v[...]
    index = sidx_v[...]
    scales = jnp.zeros(index.shape, F32)
    for level in range(levels):
        scales = jnp.where(index == level, table_s[level], scales)
    scale_ref[...] = scales
    rlow[...] = cur[...].astype(BF16)
    cols = 256

    def screen(begin, n_pieces):
        for k in range(n_pieces):
            load(begin + k).wait()
        size = n_pieces * piece
        start = begin * piece
        at = pl.ds(pl.multiple_of(start, piece), size)
        left = rlow[:, at]
        for j in range(width // cols):
            lane = slice(j * cols, (j + 1) * cols)
            block = []
            for n in range(size // per_group):
                sub = pl.ds(pl.multiple_of(start + n * per_group, per_group), per_group)
                scale = scale_ref[pl.ds(begin * (piece // per_group) + n, 1), lane]
                block.append(x_ref[sub, lane].astype(F32) * scale)
            block = jnp.concatenate(block, axis=0).astype(BF16)
            x_ref[at, lane] = block
            part[:, lane] += dot(left, block)

    mk("screen1")
    screen(0, 1)
    mk("barrier")
    pl.when(is_owner)(lambda: pl.semaphore_wait(barrier, N - 1))
    pl.when(jnp.logical_not(is_owner))(lambda: pl.semaphore_wait(barrier, V - 1 + (S - 1) * (1 + O)))
    for v in all_var:
        send(ids_all.at[mv], ids_all.at[mv], IDS, v, ms, IQ + my_q)

    mk("inv")
    for c in pulls[5:]:
        c.wait()
    for b in range(blocks):
        inv[0, b] = binv_v[b].astype(BF16)

    def hand_over():
        send(beta_v, beta_two, BETA, taker, ms)
        send(inv.at[0], inv.at[1], INV, taker, ms)

    pl.when(gives)(hand_over)

    def keep():
        beta_two[...] = beta_v[...]
        inv[1] = inv[0]

    pl.when(keeps)(keep)
    mk("screen2")
    pairs = (n_loads - 1) // 2

    def two(i, c):
        screen(1 + 2 * i, 2)
        return c

    lax.fori_loop(0, pairs, two, 0)
    if 1 + 2 * pairs < n_loads:
        screen(n_loads - 1, 1)
    recv_p[ms] = part[...]
    line = lax.broadcasted_iota(jnp.int32, (V, fit), 0)
    eight = lax.broadcasted_iota(jnp.int32, (8, fit), 0)
    turn = lax.broadcasted_iota(jnp.int32, (pad, fit), 0).astype(F32)
    lane_no = lax.broadcasted_iota(jnp.int32, (LANES, pad), 0).astype(F32)

    def place_half(hh, ss):
        first_g = 8 * hh + 4 * ss
        column = jnp.zeros((8, fit), jnp.int32)
        for i in range(4):
            column = jnp.where(eight == i, ids_all[first_g + i], column)
        column = column - mv * width
        held = (column >= 0) & (column < width)
        serial = dot(jnp.where(held, 1.0, 0.0).astype(BF16), tri[...])
        serial = jnp.where(held, serial, -1.0)
        column = jnp.where(held, column, 0)
        for i in range(4):
            col = column[i:i + 1]
            digits = jnp.where(
                eight == 0, lax.shift_right_logical(col, 7),
                jnp.where(eight == 1, col & 127, jnp.where(eight == 2, 1, 0)),
            ).astype(F32).astype(BF16)
            place = jnp.where(turn == serial[i:i + 1], 1.0, 0.0).astype(BF16)
            found = dot(digits, place, NT)
            here = found[2:3] > 0.5
            at = pl.ds(pl.multiple_of((first_g + i) * pad, pad), pad)
            high_t[:, at] = jnp.broadcast_to(jnp.where(here, found[0:1], -1.0), (ph, pad))
            low[:, at] = jnp.where(lane_no == jnp.where(here, found[1:2], -1.0), 1.0, 0.0).astype(BF16)

    mk(None)

    def own_slots():
        mk("own")
        mine = ids_all[my_g][0:1] - line * width
        marks = jnp.where((mine >= 0) & (mine < width), 1.0, 0.0)
        before = dot(marks.astype(BF16), tri[...])
        position = jnp.sum(marks * before, axis=0, keepdims=True)
        place_v[...] = jnp.where(turn == position, 1.0, 0.0).astype(BF16)
        marks_v[...] = marks
        mk(None)

    def send_gradient(p):
        wide = jnp.concatenate([part[:, t * LANES:(t + 1) * LANES] for t in range(tiles)], axis=0).astype(BF16)
        for n, (hh, ss) in enumerate(halves):
            base = 8 * hh + 4 * ss
            at = pl.ds(pl.multiple_of(base * pad, 4 * pad), 4 * pad)
            found = dot(wide, low[:, at])
            which = high_t[:, at]
            out = jnp.zeros((ph, 4 * pad), F32)
            for t in range(tiles):
                out = jnp.where(which == float(t), found[t * ph:(t + 1) * ph], out)
            out = out.astype(BF16)
            for k in range(4):
                send_a[p, base + k] = out[:, k * pad:(k + 1) * pad]
            v = 8 * hh + 2 * (1 + ss) + 1
            last = n == len(halves) - 1
            turns = [lax.rem(ms + d, 4) for d in (2, 3, 1)]
            for r in turns if last else turns + [lax.rem(ms, 4)]:
                send(send_a.at[p, base + r], recv_a.at[p, me], A + p, v, r)

        def away():
            send(send_a.at[p, my_g], recv_a.at[p, me], A + p, taker, lax.rem(ms, 4))

        unless(serves, away)

        def stay():
            recv_a[p, me] = send_a[p, my_g]

        pl.when(serves)(stay)

    def wait_sums(p):
        owner_only(lambda: got(recv_s.at[p, pl.ds(0, S * O - 1)], SM + p))
        other_only(lambda: got(recv_s.at[p, pl.ds(0, S * O)], SM + p))

    lane = lax.broadcasted_iota(jnp.int32, (ph, LANES), 1)
    sub = lax.broadcasted_iota(jnp.int32, (ph, LANES), 0)

    def length(p):
        wait_sums(p)
        total = recv_s[p, 0]
        for k in range(1, S * O):
            total = total + recv_s[p, k]
        total = jnp.broadcast_to(total, (ph, LANES))
        cross = jnp.sum(jnp.where(lane == sub, total, 0.0), axis=1, keepdims=True)
        square = jnp.sum(jnp.where(lane == sub + ph, total, 0.0), axis=1, keepdims=True)
        return cross / (square + EPSILON)

    def advance(factor, p, dst):
        for q in range(O):
            at = slice(q * chunk, (q + 1) * chunk)
            dst[:, at] = cur[:, at] - factor * recv_u[p, q].astype(F32)

    def serve(p, factor):
        mk("gotA")
        got(recv_a.at[p, pl.ds(0, N - 1)], A + p)
        mk("serve")
        if p == 0:
            def take():
                got(beta_two, BETA)
                got(inv.at[1], INV)

            unless(keeps, take)
            coef[...] = jnp.zeros(coef.shape, F32)
            coef[:, 0:kept] = beta_two[...]
        stack = []
        for v in range(V):
            val = recv_a[p, v].astype(F32)
            for s in range(1, S):
                val = val + recv_a[p, s * V + v].astype(F32)
            high = val.astype(BF16).astype(F32)
            stack += [high, val - high]
        found = dot(jnp.concatenate(stack, axis=0).astype(BF16), place_v[...])
        slots = jnp.zeros((ph, fit), F32)
        for v in range(V):
            both = found[2 * v * ph:(2 * v + 1) * ph] + found[(2 * v + 1) * ph:(2 * v + 2) * ph]
            slots = slots + marks_v[v:v + 1] * both
        slots = slots * inv_root
        if p > 0:
            slots = grad[...] - factor * slots
            coef[...] = coef[...] + factor * direct[p - 1].astype(F32)
        grad[...] = slots
        inner = slots - PENALTY * coef[...]
        ways = []
        for b in range(blocks):
            cut = slice(b * bsize, (b + 1) * bsize)
            ways.append(joined(dot(split(inner[:, cut]), inv[1, b], NT)).astype(BF16))
        way = jnp.concatenate(ways, axis=1)
        direct[p] = way
        way = way.astype(F32)
        spread = jnp.concatenate([way * marks_v[v:v + 1] for v in range(V)], axis=0).astype(BF16)
        back = dot(spread, place_v[...], NT).astype(BF16)
        for v in range(V):
            send_b[p, v] = back[v * ph:(v + 1) * ph]
        mk("sendB")
        for s in samps + [ms]:
            for v in all_var:
                send(send_b.at[p, v], recv_b.at[p, my_g], B + p, v, s)
        for s in samps:
            send(send_b.at[p, mv], recv_b.at[p, my_g], B + p, mv, s)
        recv_b[p, my_g] = send_b[p, mv]
        mk(None)

    def tell_direct(p):
        for s in samps:
            send(direct.at[p], recv_d.at[p], D + p, my_g, s)

        def away():
            send(direct.at[p], recv_d.at[p], D + p, my_g, ms)

        unless(keeps, away)

        def stay():
            recv_d[p] = direct[p]

        pl.when(keeps)(stay)

    def reduce(p):
        mk("gotC")
        got(recv_c.at[p, pl.ds(0, V - 1)], C + p)
        mk("sumC")
        val = recv_c[p, 0].astype(F32)
        for v in range(1, V):
            val = val + recv_c[p, v].astype(F32)
        low_u = (val * inv_root).astype(BF16)
        recv_u[p, my_q] = low_u

        def tell_update():
            for v in all_var:
                send(recv_u.at[p, my_q], recv_u.at[p, my_q], U + p, v, ms, UQ + p * O + my_q)

        def tell_sums():
            upd = low_u.astype(F32)
            now = cur[:, pl.ds(pl.multiple_of(my_q * chunk, chunk), chunk)]
            cross = jnp.sum(now * upd, axis=1, keepdims=True)
            square = jnp.sum(upd * upd, axis=1, keepdims=True)
            both = jnp.where(lane == sub, cross, jnp.where(lane == sub + ph, square, 0.0))
            slot = ms * O + my_q
            recv_s[p, slot] = jnp.sum(both, axis=0, keepdims=True)
            for s in samps + [ms]:
                for v in all_var:
                    send(recv_s.at[p, slot], recv_s.at[p, slot], SM + p, v, s)
            for s in samps:
                send(recv_s.at[p, slot], recv_s.at[p, slot], SM + p, mv, s)

        if p + 1 < PASSES:
            tell_update()
            tell_sums()
        else:
            tell_sums()
            tell_update()
        mk(None)

    turned = 2 * LANES

    def turn_rows(i, c):
        at = pl.ds(pl.multiple_of(i * turned, turned), turned)
        for j in range(width // turned):
            cut = slice(j * turned, (j + 1) * turned)
            xt_ref[cut, at] = x_ref[at, cut].T
        return c

    for n, (hh, ss) in enumerate(reversed(halves)):
        mk("idswait")
        got(ids_all.at[pl.ds(0, 3 if n == 0 else 4)], IQ + 2 * hh + ss)
        mk("idsproc")
        place_half(hh, ss)
        mk(None)
        if n == 0:
            pl.when(serves)(own_slots)
    factors = []
    for p in range(PASSES):
        mk("gather")
        send_gradient(p)
        mk("mid")
        if p == 0:
            mk("turn")
            lax.fori_loop(0, rows // turned, turn_rows, 0)
            mk("mid")
        if p == 1:
            got(recv_p.at[pl.ds(0, S - 1)], SC)
            val = recv_p[0]
            for s in range(1, S):
                val = val + recv_p[s]
            scores_out[...] = val * inv_root
        if p > 0:
            factors.append(length(p - 1))
        factor = factors[-1] if p else None
        mk(None)
        pl.when(serves)(functools.partial(serve, p, factor))
        mk("adv")
        if p > 0:
            advance(factor, p - 1, cur)
        mk("waitB")
        pl.when(serves)(lambda: got(recv_b.at[p, pl.ds(0, V - 1)], B + p))
        unless(serves, lambda: got(recv_b.at[p], B + p))
        mk("spread")
        way = jnp.concatenate([recv_b[p, g] for g in range(V)], axis=1).astype(F32)
        which = high_t[...]
        wide = jnp.concatenate([jnp.where(which == float(t), way, 0.0) for t in range(tiles)], axis=0)
        found = dot(wide.astype(BF16), low[...], NT).astype(BF16)
        for t in range(tiles):
            d_held[:, t * LANES:(t + 1) * LANES] = found[t * ph:(t + 1) * ph]
        mk("upd")

        for k, (v, q) in enumerate(owners):
            at = pl.ds(pl.multiple_of(q * chunk, chunk), chunk)
            send_c[p, q] = dot(d_held[...], xt_ref[:, at]).astype(BF16)
            if k < O - 1:
                send(send_c.at[p, q], recv_c.at[p, mv], C + p, v, ms)
            else:
                def away(q=q, v=v):
                    send(send_c.at[p, q], recv_c.at[p, mv], C + p, v, ms)

                other_only(away)

                def stay(q=q):
                    recv_c[p, mv] = send_c[p, q]

                owner_only(stay)
        pl.when(serves)(functools.partial(tell_direct, p))
        if p == 0:
            for s in samps:
                send(recv_p.at[ms], recv_p.at[ms], SC, mv, s)
        mk(None)
        owner_only(functools.partial(reduce, p))
        mk("waitU")
        for k, (v, q) in enumerate(reversed(owners)):
            def arrive(q=q):
                got(recv_u.at[p, q], UQ + p * O + q)

            if k == 0:
                other_only(arrive)
            else:
                arrive()
            if p + 1 < PASSES:
                at = pl.ds(pl.multiple_of(q * chunk, chunk), chunk)
                new = dot(recv_u[p, q], x_ref[at, :])
                if k == 0:
                    part[...] = new
                else:
                    part[...] += new

    mk("fin")
    factors.append(length(PASSES - 1))
    factor = factors[-1]
    advance(factor, PASSES - 1, resid_out)

    coef_out[...] = jnp.zeros((ph, fit), F32)
    coef_out[:, 0:kept] = beta_v[...]
    val = coef_out[...]
    for p in range(PASSES):
        unless(keeps, functools.partial(lambda p: got(recv_d.at[p], D + p), p))
        val = val + factors[p] * recv_d[p].astype(F32)
    coef_out[...] = val
    mk("drain")

    sent(ids_all.at[pl.ds(0, V - 1)], IDS)
    sent(recv_p.at[pl.ds(0, S - 1)], SC)

    def drain_a(p):
        pl.when(serves)(lambda: sent(recv_a.at[p, pl.ds(0, V - 1)], A + p))
        unless(serves, lambda: sent(recv_a.at[p, pl.ds(0, V)], A + p))

    def drain_serve():
        for p in range(PASSES):
            sent(recv_a.at[p, pl.ds(0, N - 1)], B + p)
            pl.when(keeps)(functools.partial(lambda p: sent(blank.at[pl.ds(0, S - 1)], D + p), p))
            unless(keeps, functools.partial(lambda p: sent(blank, D + p), p))

    def drain_owner():
        for p in range(PASSES):
            sent(send_c.at[p, pl.ds(0, O - 1)], C + p)
            sent(recv_c.at[p, pl.ds(0, V - 1)], U + p)
            sent(recv_s.at[p, pl.ds(0, N - 1)], SM + p)

    def drain_other():
        for p in range(PASSES):
            sent(send_c.at[p], C + p)

    def drain_gives():
        sent(beta_v, BETA)
        sent(inv.at[0], INV)

    for p in range(PASSES):
        drain_a(p)
    pl.when(serves)(drain_serve)
    owner_only(drain_owner)
    pl.when(gives)(drain_gives)
    other_only(drain_other)


def on_device(geno, scale_index, scale_table, residual, beta_active, block_inverse, active_ids, admit_ids):
    V, S = lax.axis_size("var"), lax.axis_size("samp")
    N = V * S
    O = V // 4
    assert V % 8 == 0 and S >= 4
    rows, width = geno.shape
    ph = residual.shape[0]
    fit = active_ids.shape[0] + admit_ids.shape[0]
    pad = LANES * pl.cdiv(2 * fit // V, LANES)
    chunk = rows // O
    vmem = pl.BlockSpec(memory_space=pltpu.VMEM)
    hbm = pl.BlockSpec(memory_space=pl.ANY)
    n_send = 4 + 6 * PASSES
    n_recv = n_send + PASSES * O + O
    per_group = rows // scale_index.shape[0]
    out = pl.pallas_call(
        functools.partial(kernel, V, S, pad),
        out_shape=(pltpu.VMEM((ph, width), F32), pltpu.VMEM((ph, fit), F32), pltpu.VMEM((ph, rows), F32)),
        in_specs=[hbm] * 8,
        out_specs=(vmem, vmem, vmem),
        scratch_shapes=[
            pltpu.VMEM((rows, width), BF16),
            pltpu.VMEM((width, rows), BF16),
            pltpu.VMEM(scale_index.shape, jnp.int32),
            pltpu.SMEM(scale_table.shape, F32),
            pltpu.VMEM((ph, rows), F32),
            pltpu.VMEM(beta_active.shape, F32),
            pltpu.VMEM(block_inverse.shape, F32),
            pltpu.VMEM((1, active_ids.shape[0]), jnp.int32),
            pltpu.VMEM((1, admit_ids.shape[0]), jnp.int32),
            pltpu.VMEM(scale_index.shape, F32),
            pltpu.VMEM((ph, rows), BF16),
            pltpu.VMEM((ph, width), F32),
            pltpu.VMEM((LANES, V * pad), BF16),
            pltpu.VMEM((ph, V * pad), F32),
            pltpu.VMEM((V, fit), F32),
            pltpu.VMEM((pad, fit), BF16),
            pltpu.VMEM((fit, fit), BF16),
            pltpu.VMEM((2,) + block_inverse.shape, BF16),
            pltpu.VMEM(beta_active.shape, F32),
            pltpu.VMEM((V, 1, fit), jnp.int32),
            pltpu.VMEM((S, ph, fit), BF16),
            pltpu.VMEM((ph, width), BF16),
            pltpu.VMEM((ph, fit), F32),
            pltpu.VMEM((ph, fit), F32),
            pltpu.VMEM((PASSES, ph, fit), BF16),
            pltpu.VMEM((PASSES, V, ph, pad), BF16),
            pltpu.VMEM((PASSES, N, ph, pad), BF16),
            pltpu.VMEM((PASSES, V, ph, pad), BF16),
            pltpu.VMEM((PASSES, V, ph, pad), BF16),
            pltpu.VMEM((PASSES, O, ph, chunk), BF16),
            pltpu.VMEM((PASSES, V, ph, chunk), BF16),
            pltpu.VMEM((PASSES, O, ph, chunk), BF16),
            pltpu.VMEM((S, ph, width), F32),
            pltpu.VMEM((PASSES, N, 1, LANES), F32),
            pltpu.VMEM((PASSES, ph, fit), BF16),
            pltpu.SemaphoreType.DMA((rows // (2 * per_group),)),
            pltpu.SemaphoreType.DMA((7,)),
            pltpu.SemaphoreType.DMA((n_send,)),
            pltpu.SemaphoreType.DMA((n_recv,)),
        ],
        compiler_params=pltpu.CompilerParams(
            collective_id=0, has_side_effects=True, vmem_limit_bytes=60 * 1024 * 1024
        ),
    )(geno, scale_index, scale_table, residual, beta_active, block_inverse, active_ids[None], admit_ids[None])

    def hand_out(*refs):
        half = len(refs) // 2
        for a, b in zip(refs[:half], refs[half:]):
            b[...] = a[...]

    return pl.pallas_call(
        hand_out, out_shape=tuple(jax.ShapeDtypeStruct(o.shape, o.dtype) for o in out),
        in_specs=[vmem] * 3, out_specs=(vmem,) * 3,
        compiler_params=pltpu.CompilerParams(vmem_limit_bytes=1024 * 1024),
    )(*out)


def solution(mesh):
    placed = (
        P("samp", "var"), P("samp", "var"), P(), P(None, "samp"), P(None, "var"),
        P("var", None, None), P("var"), P("var"),
    )
    return jax.shard_map(
        on_device, mesh=mesh, in_specs=placed,
        out_specs=(P(None, "var"), P(None, "var"), P(None, "samp")), check_vma=False,
    )
```

```python
import functools
import math

import jax
import jax.numpy as jnp
from jax import lax
from jax.experimental import pallas as pl
from jax.experimental.pallas import tpu as pltpu
from jax.sharding import PartitionSpec as P

PASSES = 3
SHARES = (0, 1, 3, 4, 7, 8)
PENALTY = 0.5
EPSILON = 1e-06
LANES = 128
F32 = jnp.float32
BF16 = jnp.bfloat16
NN = (((1,), (0,)), ((), ()))
NT = (((1,), (1,)), ((), ()))


def dot(a, b, dims=NN):
    return lax.dot_general(a, b, dims, preferred_element_type=F32)


def split(x):
    high = x.astype(BF16).astype(F32)
    return jnp.concatenate([high, x - high], axis=0).astype(BF16)


def joined(x):
    half = x.shape[0] // 2
    return x[:half] + x[half:]


def kernel(
    V, S, pad,
    geno, sidx, table, resid, beta, binv, active, admit,
    scores_out, coef_out, resid_out,
    x_ref, xt_ref, pick, xc_ref, xct_ref, part_c, sidx_v, table_s, cur, beta_v, binv_v, act_v, adm_v,
    scale_ref, rlow, part, low, high_t, marks_v, place_v, tri, inv, beta_two, ids_all, blank,
    d_held, coef, grad, direct,
    send_a, recv_a, send_b, recv_b, send_c, recv_c, recv_u, recv_p, recv_s, recv_d,
    load_sem, in_sem, send_sem, recv_sem,
):
    cur_scope = [None]

    def mk(name):
        pass

    N = V * S
    H, O = V // 8, V // 4
    rows, width = x_ref.shape
    groups = sidx_v.shape[0]
    per_group = rows // groups
    levels = table_s.shape[0]
    ph = cur.shape[0]
    kept = act_v.shape[1]
    fit = kept + adm_v.shape[1]
    blocks, bsize = binv_v.shape[0], binv_v.shape[1]
    chunk = rows // O
    tiles = width // LANES
    piece = 2 * per_group
    n_loads = rows // piece
    inv_root = 1.0 / math.sqrt(rows * S)
    mv, ms = lax.axis_index("var"), lax.axis_index("samp")
    me = ms * V + mv

    mk("greet")
    barrier = pltpu.get_barrier_semaphore()

    samps = [lax.rem(ms + d, S) for d in range(1, S)]
    if S == 4:
        samps = [3 - ms] + [ms + d - 2 * d * lax.rem(lax.div(ms, d), 2) for d in (2, 1)]

    h, z, c0 = lax.div(mv, 8), lax.rem(lax.div(mv, 2), 4), lax.rem(mv, 2)
    side = lax.div(z, 2)
    hs = [lax.rem(h + d, H) for d in range(1, H)] + [h]
    halves = [(hh, ss) for hh in hs for ss in (1 - side, side)]
    owners = [(8 * hh + 2 * (1 + ss) + 1, 2 * hh + ss) for hh, ss in halves]
    is_owner = jnp.logical_and(z == 1 + side, c0 == 1)
    my_q = 2 * h + side
    my_g = 8 * h + 4 * side + lax.rem(ms, 4)
    serves = jnp.logical_and(is_owner, ms < 4)
    own_turn = ms == 2 * lax.rem(z, 2) + c0
    keeps = jnp.logical_and(is_owner, own_turn)
    gives = jnp.logical_and(own_turn, jnp.logical_not(is_owner))
    taker = 8 * h + 2 * (1 + side) + 1
    z0 = z + side * (3 - 2 * z)
    zs = [side * 3 + (1 - 2 * side) * k for k in (3, 2, 1 - z0, z0)]
    all_var = [8 * hh + 2 * zz + cc for hh in hs for zz in zs for cc in (1 - c0, c0)][:-1]

    def hello(v, s):
        pl.semaphore_signal(
            barrier, inc=1, device_id={"var": v, "samp": s}, device_id_type=pl.DeviceIdType.MESH
        )

    for v in all_var:
        hello(v, ms)
    for s in samps:
        hello(mv, s)

    def greet_all():
        for s in samps:
            for v in all_var:
                hello(v, s)

    pl.when(is_owner)(greet_all)

    def greet_owners():
        for s in samps:
            for v, _ in owners:
                hello(v, s)

    pl.when(jnp.logical_not(is_owner))(greet_owners)
    mk("start")

    def load(i):
        at = pl.ds(pl.multiple_of(i * piece, piece), piece)
        return pltpu.make_async_copy(geno.at[at], x_ref.at[at], load_sem.at[i])

    small = [(table, table_s), (sidx, sidx_v), (resid, cur), (active, act_v), (admit, adm_v), (beta, beta_v), (binv, binv_v)]
    pulls = [pltpu.make_async_copy(a, b, in_sem.at[i]) for i, (a, b) in enumerate(small)]
    for c in pulls[:5]:
        c.start()
    load(0).start()
    for c in pulls[5:]:
        c.start()


    def owner_only(fn):
        pl.when(is_owner)(fn)

    def other_only(fn):
        pl.when(jnp.logical_not(is_owner))(fn)

    def unless(cond, fn):
        pl.when(jnp.logical_not(cond))(fn)

    def send(src, dst, sem, v, s, r_sem=None):
        pltpu.make_async_remote_copy(
            src_ref=src, dst_ref=dst, send_sem=send_sem.at[sem],
            recv_sem=recv_sem.at[sem if r_sem is None else r_sem],
            device_id={"var": v, "samp": s}, device_id_type=pl.DeviceIdType.MESH,
        ).start()

    def got(ref, sem):
        pltpu.make_async_copy(ref, ref, recv_sem.at[sem]).wait()

    def sent(ref, sem):
        pltpu.make_async_copy(ref, ref, send_sem.at[sem]).wait()

    IDS, INV, BETA, SC = 0, 1, 2, 3
    A = 4
    B = A + PASSES
    C = B + PASSES
    SM = C + PASSES
    D = SM + PASSES
    U = D + PASSES
    UQ = U + PASSES
    IQ = UQ + PASSES * O

    tri[...] = jnp.where(
        lax.broadcasted_iota(jnp.int32, (fit, fit), 0) < lax.broadcasted_iota(jnp.int32, (fit, fit), 1),
        1.0, 0.0,
    ).astype(BF16)
    part[...] = jnp.zeros((ph, width), F32)
    mk("inputs")
    for c in pulls[:5]:
        c.wait()
    mk("setup")
    for i in range(1, n_loads):
        load(i).start()
    ids_all[mv, :, 0:kept] = act_v[...]
    ids_all[mv, :, kept:fit] = adm_v[...]
    index = sidx_v[...]
    scales = jnp.zeros(index.shape, F32)
    for level in range(levels):
        scales = jnp.where(index == level, table_s[level], scales)
    scale_ref[...] = scales
    rlow[...] = cur[...].astype(BF16)
    cols = 256

    def screen(begin, n_pieces):
        for k in range(n_pieces):
            load(begin + k).wait()
        size = n_pieces * piece
        start = begin * piece
        at = pl.ds(pl.multiple_of(start, piece), size)
        left = rlow[:, at]
        for j in range(width // cols):
            lane = slice(j * cols, (j + 1) * cols)
            block = []
            for n in range(size // per_group):
                sub = pl.ds(pl.multiple_of(start + n * per_group, per_group), per_group)
                scale = scale_ref[pl.ds(begin * (piece // per_group) + n, 1), lane]
                block.append(x_ref[sub, lane].astype(F32) * scale)
            block = jnp.concatenate(block, axis=0).astype(BF16)
            x_ref[at, lane] = block
            part[:, lane] += dot(left, block)

    mk("screen1")
    screen(0, 1)
    mk("barrier")
    pl.when(is_owner)(lambda: pl.semaphore_wait(barrier, N - 1))
    pl.when(jnp.logical_not(is_owner))(lambda: pl.semaphore_wait(barrier, V - 1 + (S - 1) * (1 + O)))
    for v in all_var:
        send(ids_all.at[mv], ids_all.at[mv], IDS, v, ms, IQ + my_q)

    mk("inv")
    for c in pulls[5:]:
        c.wait()
    for b in range(blocks):
        inv[0, b] = binv_v[b].astype(BF16)

    def hand_over():
        send(beta_v, beta_two, BETA, taker, ms)
        send(inv.at[0], inv.at[1], INV, taker, ms)

    pl.when(gives)(hand_over)

    def keep():
        beta_two[...] = beta_v[...]
        inv[1] = inv[0]

    pl.when(keeps)(keep)
    mk("screen2")
    pairs = (n_loads - 1) // 2

    def two(i, c):
        screen(1 + 2 * i, 2)
        return c

    lax.fori_loop(0, pairs, two, 0)
    if 1 + 2 * pairs < n_loads:
        screen(n_loads - 1, 1)
    recv_p[ms] = part[...]
    line = lax.broadcasted_iota(jnp.int32, (V, fit), 0)
    eight = lax.broadcasted_iota(jnp.int32, (8, fit), 0)
    turn = lax.broadcasted_iota(jnp.int32, (pad, fit), 0).astype(F32)
    lane_no = lax.broadcasted_iota(jnp.int32, (LANES, pad), 0).astype(F32)

    def place_half(hh, ss):
        first_g = 8 * hh + 4 * ss
        column = jnp.zeros((8, fit), jnp.int32)
        for i in range(4):
            column = jnp.where(eight == i, ids_all[first_g + i], column)
        column = column - mv * width
        held = (column >= 0) & (column < width)
        serial = dot(jnp.where(held, 1.0, 0.0).astype(BF16), tri[...])
        serial = jnp.where(held, serial, -1.0)
        column = jnp.where(held, column, 0)
        for i in range(4):
            col = column[i:i + 1]
            digits = jnp.where(
                eight == 0, lax.shift_right_logical(col, 7),
                jnp.where(eight == 1, col & 127, jnp.where(eight == 2, 1, 0)),
            ).astype(F32).astype(BF16)
            place = jnp.where(turn == serial[i:i + 1], 1.0, 0.0).astype(BF16)
            found = dot(digits, place, NT)
            here = found[2:3] > 0.5
            at = pl.ds(pl.multiple_of((first_g + i) * pad, pad), pad)
            high_t[:, at] = jnp.broadcast_to(jnp.where(here, found[0:1], -1.0), (ph, pad))
            low[:, at] = jnp.where(lane_no == jnp.where(here, found[1:2], -1.0), 1.0, 0.0).astype(BF16)

    mk(None)

    def own_slots():
        mk("own")
        mine = ids_all[my_g][0:1] - line * width
        marks = jnp.where((mine >= 0) & (mine < width), 1.0, 0.0)
        before = dot(marks.astype(BF16), tri[...])
        position = jnp.sum(marks * before, axis=0, keepdims=True)
        place_v[...] = jnp.where(turn == position, 1.0, 0.0).astype(BF16)
        marks_v[...] = marks
        mk(None)

    marks_at = [c * n_loads // 8 for c in SHARES]

    def build_pick():
        for t in range(tiles):
            one = jnp.where(high_t[0:1, :] == float(t), low[...].astype(F32), 0.0)
            pick[t * LANES:(t + 1) * LANES, :] = one.astype(BF16)

    def compact_piece(i, c):
        at = pl.ds(pl.multiple_of(i * piece, piece), piece)
        block = dot(x_ref[at, :], pick[...]).astype(BF16)
        xc_ref[at, :] = block
        for j in range(V * pad // turned):
            cut = slice(j * turned, (j + 1) * turned)
            xct_ref[cut, at] = xc_ref[at, cut].T
        return c

    def compact(k):
        lax.fori_loop(marks_at[k], marks_at[k + 1], compact_piece, 0)

    turned = 2 * LANES

    def send_gradient(p):
        done = p == PASSES - 1
        if done:
            for g in range(V):
                send_a[p, g] = part_c[:, g * pad:(g + 1) * pad].astype(BF16)
        else:
            wide = jnp.concatenate([part[:, t * LANES:(t + 1) * LANES] for t in range(tiles)], axis=0).astype(BF16)
        for n, (hh, ss) in enumerate(halves):
            base = 8 * hh + 4 * ss
            if not done:
                at = pl.ds(pl.multiple_of(base * pad, 4 * pad), 4 * pad)
                found = dot(wide, low[:, at])
                which = high_t[:, at]
                out = jnp.zeros((ph, 4 * pad), F32)
                for t in range(tiles):
                    out = jnp.where(which == float(t), found[t * ph:(t + 1) * ph], out)
                out = out.astype(BF16)
                for k in range(4):
                    send_a[p, base + k] = out[:, k * pad:(k + 1) * pad]
            v = 8 * hh + 2 * (1 + ss) + 1
            last = n == len(halves) - 1
            turns = [lax.rem(ms + d, 4) for d in (2, 3, 1)]
            for r in turns if last else turns + [lax.rem(ms, 4)]:
                send(send_a.at[p, base + r], recv_a.at[p, me], A + p, v, r)

        def away():
            send(send_a.at[p, my_g], recv_a.at[p, me], A + p, taker, lax.rem(ms, 4))

        unless(serves, away)

        def stay():
            recv_a[p, me] = send_a[p, my_g]

        pl.when(serves)(stay)

    def wait_sums(p):
        owner_only(lambda: got(recv_s.at[p, pl.ds(0, S * O - 1)], SM + p))
        other_only(lambda: got(recv_s.at[p, pl.ds(0, S * O)], SM + p))

    lane = lax.broadcasted_iota(jnp.int32, (ph, LANES), 1)
    sub = lax.broadcasted_iota(jnp.int32, (ph, LANES), 0)

    def length(p):
        wait_sums(p)
        total = recv_s[p, 0]
        for k in range(1, S * O):
            total = total + recv_s[p, k]
        total = jnp.broadcast_to(total, (ph, LANES))
        cross = jnp.sum(jnp.where(lane == sub, total, 0.0), axis=1, keepdims=True)
        square = jnp.sum(jnp.where(lane == sub + ph, total, 0.0), axis=1, keepdims=True)
        return cross / (square + EPSILON)

    def advance(factor, p, dst):
        for q in range(O):
            at = slice(q * chunk, (q + 1) * chunk)
            dst[:, at] = cur[:, at] - factor * recv_u[p, q].astype(F32)

    def serve(p, factor):
        mk("gotA")
        got(recv_a.at[p, pl.ds(0, N - 1)], A + p)
        mk("serve")
        if p == 0:
            def take():
                got(beta_two, BETA)
                got(inv.at[1], INV)

            unless(keeps, take)
            coef[...] = jnp.zeros(coef.shape, F32)
            coef[:, 0:kept] = beta_two[...]
        stack = []
        for v in range(V):
            val = recv_a[p, v].astype(F32)
            for s in range(1, S):
                val = val + recv_a[p, s * V + v].astype(F32)
            high = val.astype(BF16).astype(F32)
            stack += [high, val - high]
        found = dot(jnp.concatenate(stack, axis=0).astype(BF16), place_v[...])
        slots = jnp.zeros((ph, fit), F32)
        for v in range(V):
            both = found[2 * v * ph:(2 * v + 1) * ph] + found[(2 * v + 1) * ph:(2 * v + 2) * ph]
            slots = slots + marks_v[v:v + 1] * both
        slots = slots * inv_root
        if p > 0:
            slots = grad[...] - factor * slots
            coef[...] = coef[...] + factor * direct[p - 1].astype(F32)
        grad[...] = slots
        inner = slots - PENALTY * coef[...]
        ways = []
        for b in range(blocks):
            cut = slice(b * bsize, (b + 1) * bsize)
            ways.append(joined(dot(split(inner[:, cut]), inv[1, b], NT)).astype(BF16))
        way = jnp.concatenate(ways, axis=1)
        direct[p] = way
        way = way.astype(F32)
        spread = jnp.concatenate([way * marks_v[v:v + 1] for v in range(V)], axis=0).astype(BF16)
        back = dot(spread, place_v[...], NT).astype(BF16)
        for v in range(V):
            send_b[p, v] = back[v * ph:(v + 1) * ph]
        mk("sendB")
        for s in samps + [ms]:
            for v in all_var:
                send(send_b.at[p, v], recv_b.at[p, my_g], B + p, v, s)
        for s in samps:
            send(send_b.at[p, mv], recv_b.at[p, my_g], B + p, mv, s)
        recv_b[p, my_g] = send_b[p, mv]
        mk(None)

    def tell_direct(p):
        for s in samps:
            send(direct.at[p], recv_d.at[p], D + p, my_g, s)

        def away():
            send(direct.at[p], recv_d.at[p], D + p, my_g, ms)

        unless(keeps, away)

        def stay():
            recv_d[p] = direct[p]

        pl.when(keeps)(stay)

    def reduce(p):
        mk("gotC")
        got(recv_c.at[p, pl.ds(0, V - 1)], C + p)
        mk("sumC")
        val = recv_c[p, 0].astype(F32)
        for v in range(1, V):
            val = val + recv_c[p, v].astype(F32)
        low_u = (val * inv_root).astype(BF16)
        recv_u[p, my_q] = low_u

        def tell_update():
            for v in all_var:
                send(recv_u.at[p, my_q], recv_u.at[p, my_q], U + p, v, ms, UQ + p * O + my_q)

        def tell_sums():
            upd = low_u.astype(F32)
            now = cur[:, pl.ds(pl.multiple_of(my_q * chunk, chunk), chunk)]
            cross = jnp.sum(now * upd, axis=1, keepdims=True)
            square = jnp.sum(upd * upd, axis=1, keepdims=True)
            both = jnp.where(lane == sub, cross, jnp.where(lane == sub + ph, square, 0.0))
            slot = ms * O + my_q
            recv_s[p, slot] = jnp.sum(both, axis=0, keepdims=True)
            for s in samps + [ms]:
                for v in all_var:
                    send(recv_s.at[p, slot], recv_s.at[p, slot], SM + p, v, s)
            for s in samps:
                send(recv_s.at[p, slot], recv_s.at[p, slot], SM + p, mv, s)

        if p + 1 < PASSES:
            tell_update()
            tell_sums()
        else:
            tell_sums()
            tell_update()
        mk(None)

    def turn_rows(i, c):
        at = pl.ds(pl.multiple_of(i * turned, turned), turned)
        for j in range(width // turned):
            cut = slice(j * turned, (j + 1) * turned)
            xt_ref[cut, at] = x_ref[at, cut].T
        return c

    for n, (hh, ss) in enumerate(reversed(halves)):
        mk("idswait")
        got(ids_all.at[pl.ds(0, 3 if n == 0 else 4)], IQ + 2 * hh + ss)
        mk("idsproc")
        place_half(hh, ss)
        mk(None)
        if n == 0:
            pl.when(serves)(own_slots)
    factors = []
    for p in range(PASSES):
        mk("gather")
        send_gradient(p)
        mk("mid")
        if p == 0:
            mk("turn")
            lax.fori_loop(0, rows // turned, turn_rows, 0)
            mk("mid")
        if p == 1:
            mk("cmpA1")
            compact(3)
            mk("mid")
            got(recv_p.at[pl.ds(0, S - 1)], SC)
            val = recv_p[0]
            for s in range(1, S):
                val = val + recv_p[s]
            scores_out[...] = val * inv_root
        if p > 0:
            factors.append(length(p - 1))
        factor = factors[-1] if p else None
        mk(None)
        pl.when(serves)(functools.partial(serve, p, factor))
        mk("adv")
        if p > 0:
            advance(factor, p - 1, cur)
        if p < 2:
            mk("cmpB")
            if p == 0:
                build_pick()
            compact(0 if p == 0 else 4)
        mk("waitB")
        pl.when(serves)(lambda: got(recv_b.at[p, pl.ds(0, V - 1)], B + p))
        unless(serves, lambda: got(recv_b.at[p], B + p))
        mk("spread")
        way = jnp.concatenate([recv_b[p, g] for g in range(V)], axis=1)
        if p == 0:
            way = way.astype(F32)
            which = high_t[...]
            wide = jnp.concatenate([jnp.where(which == float(t), way, 0.0) for t in range(tiles)], axis=0)
            found = dot(wide.astype(BF16), low[...], NT).astype(BF16)
            for t in range(tiles):
                d_held[:, t * LANES:(t + 1) * LANES] = found[t * ph:(t + 1) * ph]
        mk("upd")

        for k, (v, q) in enumerate(owners):
            at = pl.ds(pl.multiple_of(q * chunk, chunk), chunk)
            if p == 0:
                send_c[p, q] = dot(d_held[...], xt_ref[:, at]).astype(BF16)
            else:
                send_c[p, q] = dot(way, xct_ref[:, at]).astype(BF16)
            if k < O - 1:
                send(send_c.at[p, q], recv_c.at[p, mv], C + p, v, ms)
            else:
                def away(q=q, v=v):
                    send(send_c.at[p, q], recv_c.at[p, mv], C + p, v, ms)

                other_only(away)

                def stay(q=q):
                    recv_c[p, mv] = send_c[p, q]

                owner_only(stay)
        pl.when(serves)(functools.partial(tell_direct, p))
        if p == 0:
            for s in samps:
                send(recv_p.at[ms], recv_p.at[ms], SC, mv, s)
        mk(None)
        if p == 0:
            mk("cmpC")
            compact(1)
            mk(None)
        owner_only(functools.partial(reduce, p))
        if p == 0:
            mk("cmpU")
            compact(2)
        mk("waitU")
        for k, (v, q) in enumerate(reversed(owners)):
            def arrive(q=q):
                got(recv_u.at[p, q], UQ + p * O + q)

            if k == 0:
                other_only(arrive)
            else:
                arrive()
            if p + 1 < PASSES:
                at = pl.ds(pl.multiple_of(q * chunk, chunk), chunk)
                left = PASSES - 2 - p
                new = dot(recv_u[p, q], x_ref[at, :] if left else xc_ref[at, :])
                total = part if left else part_c
                if k == 0:
                    total[...] = new
                else:
                    total[...] += new

    mk("fin")
    factors.append(length(PASSES - 1))
    factor = factors[-1]
    advance(factor, PASSES - 1, resid_out)

    coef_out[...] = jnp.zeros((ph, fit), F32)
    coef_out[:, 0:kept] = beta_v[...]
    val = coef_out[...]
    for p in range(PASSES):
        unless(keeps, functools.partial(lambda p: got(recv_d.at[p], D + p), p))
        val = val + factors[p] * recv_d[p].astype(F32)
    coef_out[...] = val
    mk("drain")

    sent(ids_all.at[pl.ds(0, V - 1)], IDS)
    sent(recv_p.at[pl.ds(0, S - 1)], SC)

    def drain_a(p):
        pl.when(serves)(lambda: sent(recv_a.at[p, pl.ds(0, V - 1)], A + p))
        unless(serves, lambda: sent(recv_a.at[p, pl.ds(0, V)], A + p))

    def drain_serve():
        for p in range(PASSES):
            sent(recv_a.at[p, pl.ds(0, N - 1)], B + p)
            pl.when(keeps)(functools.partial(lambda p: sent(blank.at[pl.ds(0, S - 1)], D + p), p))
            unless(keeps, functools.partial(lambda p: sent(blank, D + p), p))

    def drain_owner():
        for p in range(PASSES):
            sent(send_c.at[p, pl.ds(0, O - 1)], C + p)
            sent(recv_c.at[p, pl.ds(0, V - 1)], U + p)
            sent(recv_s.at[p, pl.ds(0, N - 1)], SM + p)

    def drain_other():
        for p in range(PASSES):
            sent(send_c.at[p], C + p)

    def drain_gives():
        sent(beta_v, BETA)
        sent(inv.at[0], INV)

    for p in range(PASSES):
        drain_a(p)
    pl.when(serves)(drain_serve)
    owner_only(drain_owner)
    pl.when(gives)(drain_gives)
    other_only(drain_other)


def on_device(geno, scale_index, scale_table, residual, beta_active, block_inverse, active_ids, admit_ids):
    V, S = lax.axis_size("var"), lax.axis_size("samp")
    N = V * S
    O = V // 4
    assert V % 8 == 0 and S >= 4
    rows, width = geno.shape
    ph = residual.shape[0]
    fit = active_ids.shape[0] + admit_ids.shape[0]
    pad = LANES * pl.cdiv(2 * fit // V, LANES)
    chunk = rows // O
    vmem = pl.BlockSpec(memory_space=pltpu.VMEM)
    hbm = pl.BlockSpec(memory_space=pl.ANY)
    n_send = 4 + 6 * PASSES
    n_recv = n_send + PASSES * O + O
    per_group = rows // scale_index.shape[0]
    out = pl.pallas_call(
        functools.partial(kernel, V, S, pad),
        out_shape=(pltpu.VMEM((ph, width), F32), pltpu.VMEM((ph, fit), F32), pltpu.VMEM((ph, rows), F32)),
        in_specs=[hbm] * 8,
        out_specs=(vmem, vmem, vmem),
        scratch_shapes=[
            pltpu.VMEM((rows, width), BF16),
            pltpu.VMEM((width, rows), BF16),
            pltpu.VMEM((width, V * pad), BF16),
            pltpu.VMEM((rows, V * pad), BF16),
            pltpu.VMEM((V * pad, rows), BF16),
            pltpu.VMEM((ph, V * pad), F32),
            pltpu.VMEM(scale_index.shape, jnp.int32),
            pltpu.SMEM(scale_table.shape, F32),
            pltpu.VMEM((ph, rows), F32),
            pltpu.VMEM(beta_active.shape, F32),
            pltpu.VMEM(block_inverse.shape, F32),
            pltpu.VMEM((1, active_ids.shape[0]), jnp.int32),
            pltpu.VMEM((1, admit_ids.shape[0]), jnp.int32),
            pltpu.VMEM(scale_index.shape, F32),
            pltpu.VMEM((ph, rows), BF16),
            pltpu.VMEM((ph, width), F32),
            pltpu.VMEM((LANES, V * pad), BF16),
            pltpu.VMEM((ph, V * pad), F32),
            pltpu.VMEM((V, fit), F32),
            pltpu.VMEM((pad, fit), BF16),
            pltpu.VMEM((fit, fit), BF16),
            pltpu.VMEM((2,) + block_inverse.shape, BF16),
            pltpu.VMEM(beta_active.shape, F32),
            pltpu.VMEM((V, 1, fit), jnp.int32),
            pltpu.VMEM((S, ph, fit), BF16),
            pltpu.VMEM((ph, width), BF16),
            pltpu.VMEM((ph, fit), F32),
            pltpu.VMEM((ph, fit), F32),
            pltpu.VMEM((PASSES, ph, fit), BF16),
            pltpu.VMEM((PASSES, V, ph, pad), BF16),
            pltpu.VMEM((PASSES, N, ph, pad), BF16),
            pltpu.VMEM((PASSES, V, ph, pad), BF16),
            pltpu.VMEM((PASSES, V, ph, pad), BF16),
            pltpu.VMEM((PASSES, O, ph, chunk), BF16),
            pltpu.VMEM((PASSES, V, ph, chunk), BF16),
            pltpu.VMEM((PASSES, O, ph, chunk), BF16),
            pltpu.VMEM((S, ph, width), F32),
            pltpu.VMEM((PASSES, N, 1, LANES), F32),
            pltpu.VMEM((PASSES, ph, fit), BF16),
            pltpu.SemaphoreType.DMA((rows // (2 * per_group),)),
            pltpu.SemaphoreType.DMA((7,)),
            pltpu.SemaphoreType.DMA((n_send,)),
            pltpu.SemaphoreType.DMA((n_recv,)),
        ],
        compiler_params=pltpu.CompilerParams(
            collective_id=0, has_side_effects=True, vmem_limit_bytes=60 * 1024 * 1024
        ),
    )(geno, scale_index, scale_table, residual, beta_active, block_inverse, active_ids[None], admit_ids[None])

    def hand_out(*refs):
        half = len(refs) // 2
        for a, b in zip(refs[:half], refs[half:]):
            b[...] = a[...]

    return pl.pallas_call(
        hand_out, out_shape=tuple(jax.ShapeDtypeStruct(o.shape, o.dtype) for o in out),
        in_specs=[vmem] * 3, out_specs=(vmem,) * 3,
        compiler_params=pltpu.CompilerParams(vmem_limit_bytes=1024 * 1024),
    )(*out)


def solution(mesh):
    placed = (
        P("samp", "var"), P("samp", "var"), P(), P(None, "samp"), P(None, "var"),
        P("var", None, None), P("var"), P("var"),
    )
    return jax.shard_map(
        on_device, mesh=mesh, in_specs=placed,
        out_specs=(P(None, "var"), P(None, "var"), P(None, "samp")), check_vma=False,
    )
```

```python
import functools
import math

import jax
import jax.numpy as jnp
from jax import lax
from jax.experimental import pallas as pl
from jax.experimental.pallas import tpu as pltpu
from jax.sharding import PartitionSpec as P

PASSES = 3
SHARES = (0, 1, 3, 4, 6, 8)
PENALTY = 0.5
EPSILON = 1e-06
LANES = 128
F32 = jnp.float32
BF16 = jnp.bfloat16
NN = (((1,), (0,)), ((), ()))
NT = (((1,), (1,)), ((), ()))


def dot(a, b, dims=NN):
    return lax.dot_general(a, b, dims, preferred_element_type=F32)


def split(x):
    high = x.astype(BF16).astype(F32)
    return jnp.concatenate([high, x - high], axis=0).astype(BF16)


def joined(x):
    half = x.shape[0] // 2
    return x[:half] + x[half:]


def kernel(
    V, S, pad,
    geno, sidx, table, resid, beta, binv, active, admit,
    scores_out, coef_out, resid_out,
    x_ref, xt_ref, pick, xc_ref, xct_ref, part_c, sidx_v, table_s, cur, beta_v, binv_v, act_v, adm_v,
    scale_ref, rlow, part, low, high_t, marks_v, place_v, tri, inv, beta_two, ids_all, blank,
    d_held, coef, grad, direct,
    send_a, recv_a, send_b, recv_b, send_c, recv_c, recv_u, recv_p, recv_s, recv_d,
    load_sem, in_sem, send_sem, recv_sem,
):
    cur_scope = [None]

    def mk(name):
        pass

    N = V * S
    H, O = V // 8, V // 4
    rows, width = x_ref.shape
    groups = sidx_v.shape[0]
    per_group = rows // groups
    levels = table_s.shape[0]
    ph = cur.shape[0]
    kept = act_v.shape[1]
    fit = kept + adm_v.shape[1]
    blocks, bsize = binv_v.shape[0], binv_v.shape[1]
    chunk = rows // O
    tiles = width // LANES
    piece = 2 * per_group
    n_loads = rows // piece
    inv_root = 1.0 / math.sqrt(rows * S)
    mv, ms = lax.axis_index("var"), lax.axis_index("samp")
    me = ms * V + mv

    mk("greet")
    barrier = pltpu.get_barrier_semaphore()

    samps = [lax.rem(ms + d, S) for d in range(1, S)]
    if S == 4:
        samps = [3 - ms] + [ms + d - 2 * d * lax.rem(lax.div(ms, d), 2) for d in (2, 1)]

    h, z, c0 = lax.div(mv, 8), lax.rem(lax.div(mv, 2), 4), lax.rem(mv, 2)
    side = lax.div(z, 2)
    hs = [lax.rem(h + d, H) for d in range(1, H)] + [h]
    halves = [(hh, ss) for hh in hs for ss in (1 - side, side)]
    owners = [(8 * hh + 2 * (1 + ss) + 1, 2 * hh + ss) for hh, ss in halves]
    is_owner = jnp.logical_and(z == 1 + side, c0 == 1)
    my_q = 2 * h + side
    my_g = 8 * h + 4 * side + lax.rem(ms, 4)
    serves = jnp.logical_and(is_owner, ms < 4)
    own_turn = ms == 2 * lax.rem(z, 2) + c0
    keeps = jnp.logical_and(is_owner, own_turn)
    gives = jnp.logical_and(own_turn, jnp.logical_not(is_owner))
    taker = 8 * h + 2 * (1 + side) + 1
    z0 = z + side * (3 - 2 * z)
    zs = [side * 3 + (1 - 2 * side) * k for k in (3, 2, 1 - z0, z0)]
    all_var = [8 * hh + 2 * zz + cc for hh in hs for zz in zs for cc in (1 - c0, c0)][:-1]

    def hello(v, s):
        pl.semaphore_signal(
            barrier, inc=1, device_id={"var": v, "samp": s}, device_id_type=pl.DeviceIdType.MESH
        )

    for v in all_var:
        hello(v, ms)
    for s in samps:
        hello(mv, s)

    def greet_all():
        for s in samps:
            for v in all_var:
                hello(v, s)

    pl.when(is_owner)(greet_all)

    def greet_owners():
        for s in samps:
            for v, _ in owners:
                hello(v, s)

    pl.when(jnp.logical_not(is_owner))(greet_owners)
    mk("start")

    def load(i):
        at = pl.ds(pl.multiple_of(i * piece, piece), piece)
        return pltpu.make_async_copy(geno.at[at], x_ref.at[at], load_sem.at[i])

    small = [(table, table_s), (sidx, sidx_v), (resid, cur), (active, act_v), (admit, adm_v), (beta, beta_v), (binv, binv_v)]
    pulls = [pltpu.make_async_copy(a, b, in_sem.at[i]) for i, (a, b) in enumerate(small)]
    for c in pulls[:5]:
        c.start()
    load(0).start()
    for c in pulls[5:]:
        c.start()


    def owner_only(fn):
        pl.when(is_owner)(fn)

    def other_only(fn):
        pl.when(jnp.logical_not(is_owner))(fn)

    def unless(cond, fn):
        pl.when(jnp.logical_not(cond))(fn)

    def send(src, dst, sem, v, s, r_sem=None):
        pltpu.make_async_remote_copy(
            src_ref=src, dst_ref=dst, send_sem=send_sem.at[sem],
            recv_sem=recv_sem.at[sem if r_sem is None else r_sem],
            device_id={"var": v, "samp": s}, device_id_type=pl.DeviceIdType.MESH,
        ).start()

    def got(ref, sem):
        pltpu.make_async_copy(ref, ref, recv_sem.at[sem]).wait()

    def sent(ref, sem):
        pltpu.make_async_copy(ref, ref, send_sem.at[sem]).wait()

    IDS, INV, BETA, SC = 0, 1, 2, 3
    A = 4
    B = A + PASSES
    C = B + PASSES
    SM = C + PASSES
    D = SM + PASSES
    U = D + PASSES
    UQ = U + PASSES
    IQ = UQ + PASSES * O

    tri[...] = jnp.where(
        lax.broadcasted_iota(jnp.int32, (fit, fit), 0) < lax.broadcasted_iota(jnp.int32, (fit, fit), 1),
        1.0, 0.0,
    ).astype(BF16)
    part[...] = jnp.zeros((ph, width), F32)
    mk("inputs")
    for c in pulls[:5]:
        c.wait()
    mk("setup")
    for i in range(1, n_loads):
        load(i).start()
    ids_all[mv, :, 0:kept] = act_v[...]
    ids_all[mv, :, kept:fit] = adm_v[...]
    index = sidx_v[...]
    scales = jnp.zeros(index.shape, F32)
    for level in range(levels):
        scales = jnp.where(index == level, table_s[level], scales)
    scale_ref[...] = scales
    rlow[...] = cur[...].astype(BF16)
    cols = 256

    def screen(begin, n_pieces):
        for k in range(n_pieces):
            load(begin + k).wait()
        size = n_pieces * piece
        start = begin * piece
        at = pl.ds(pl.multiple_of(start, piece), size)
        left = rlow[:, at]
        for j in range(width // cols):
            lane = slice(j * cols, (j + 1) * cols)
            block = []
            for n in range(size // per_group):
                sub = pl.ds(pl.multiple_of(start + n * per_group, per_group), per_group)
                scale = scale_ref[pl.ds(begin * (piece // per_group) + n, 1), lane]
                block.append(x_ref[sub, lane].astype(F32) * scale)
            block = jnp.concatenate(block, axis=0).astype(BF16)
            x_ref[at, lane] = block
            part[:, lane] += dot(left, block)

    mk("screen1")
    screen(0, 1)
    mk("barrier")
    pl.when(is_owner)(lambda: pl.semaphore_wait(barrier, N - 1))
    pl.when(jnp.logical_not(is_owner))(lambda: pl.semaphore_wait(barrier, V - 1 + (S - 1) * (1 + O)))
    for v in all_var:
        send(ids_all.at[mv], ids_all.at[mv], IDS, v, ms, IQ + my_q)

    mk("inv")
    for c in pulls[5:]:
        c.wait()
    for b in range(blocks):
        inv[0, b] = binv_v[b].astype(BF16)

    def hand_over():
        send(beta_v, beta_two, BETA, taker, ms)
        send(inv.at[0], inv.at[1], INV, taker, ms)

    pl.when(gives)(hand_over)

    def keep():
        beta_two[...] = beta_v[...]
        inv[1] = inv[0]

    pl.when(keeps)(keep)
    mk("screen2")
    pairs = (n_loads - 1) // 2

    def two(i, c):
        screen(1 + 2 * i, 2)
        return c

    lax.fori_loop(0, pairs, two, 0)
    if 1 + 2 * pairs < n_loads:
        screen(n_loads - 1, 1)
    recv_p[ms] = part[...]
    line = lax.broadcasted_iota(jnp.int32, (V, fit), 0)
    eight = lax.broadcasted_iota(jnp.int32, (8, fit), 0)
    turn = lax.broadcasted_iota(jnp.int32, (pad, fit), 0).astype(F32)
    lane_no = lax.broadcasted_iota(jnp.int32, (LANES, pad), 0).astype(F32)

    def place_half(hh, ss):
        first_g = 8 * hh + 4 * ss
        column = jnp.zeros((8, fit), jnp.int32)
        for i in range(4):
            column = jnp.where(eight == i, ids_all[first_g + i], column)
        column = column - mv * width
        held = (column >= 0) & (column < width)
        serial = dot(jnp.where(held, 1.0, 0.0).astype(BF16), tri[...])
        serial = jnp.where(held, serial, -1.0)
        column = jnp.where(held, column, 0)
        for i in range(4):
            col = column[i:i + 1]
            digits = jnp.where(
                eight == 0, lax.shift_right_logical(col, 7),
                jnp.where(eight == 1, col & 127, jnp.where(eight == 2, 1, 0)),
            ).astype(F32).astype(BF16)
            place = jnp.where(turn == serial[i:i + 1], 1.0, 0.0).astype(BF16)
            found = dot(digits, place, NT)
            here = found[2:3] > 0.5
            at = pl.ds(pl.multiple_of((first_g + i) * pad, pad), pad)
            high_t[:, at] = jnp.broadcast_to(jnp.where(here, found[0:1], -1.0), (ph, pad))
            low[:, at] = jnp.where(lane_no == jnp.where(here, found[1:2], -1.0), 1.0, 0.0).astype(BF16)

    mk(None)

    def own_slots():
        mk("own")
        mine = ids_all[my_g][0:1] - line * width
        marks = jnp.where((mine >= 0) & (mine < width), 1.0, 0.0)
        before = dot(marks.astype(BF16), tri[...])
        position = jnp.sum(marks * before, axis=0, keepdims=True)
        place_v[...] = jnp.where(turn == position, 1.0, 0.0).astype(BF16)
        marks_v[...] = marks
        mk(None)

    marks_at = [c * n_loads // 8 for c in SHARES]

    def build_pick():
        for t in range(tiles):
            one = jnp.where(high_t[0:1, :] == float(t), low[...].astype(F32), 0.0)
            pick[t * LANES:(t + 1) * LANES, :] = one.astype(BF16)

    def compact_piece(i, c):
        at = pl.ds(pl.multiple_of(i * piece, piece), piece)
        block = dot(x_ref[at, :], pick[...]).astype(BF16)
        xc_ref[at, :] = block
        for j in range(V * pad // turned):
            cut = slice(j * turned, (j + 1) * turned)
            xct_ref[cut, at] = xc_ref[at, cut].T
        return c

    def compact(k):
        lax.fori_loop(marks_at[k], marks_at[k + 1], compact_piece, 0)

    turned = 2 * LANES

    def send_gradient(p):
        done = p == PASSES - 1
        if done:
            for g in range(V):
                send_a[p, g] = part_c[:, g * pad:(g + 1) * pad].astype(BF16)
        else:
            wide = jnp.concatenate([part[:, t * LANES:(t + 1) * LANES] for t in range(tiles)], axis=0).astype(BF16)
        for n, (hh, ss) in enumerate(halves):
            base = 8 * hh + 4 * ss
            if not done:
                at = pl.ds(pl.multiple_of(base * pad, 4 * pad), 4 * pad)
                found = dot(wide, low[:, at])
                which = high_t[:, at]
                out = jnp.zeros((ph, 4 * pad), F32)
                for t in range(tiles):
                    out = jnp.where(which == float(t), found[t * ph:(t + 1) * ph], out)
                out = out.astype(BF16)
                for k in range(4):
                    send_a[p, base + k] = out[:, k * pad:(k + 1) * pad]
            v = 8 * hh + 2 * (1 + ss) + 1
            last = n == len(halves) - 1
            turns = [lax.rem(ms + d, 4) for d in (2, 3, 1)]
            for r in turns if last else turns + [lax.rem(ms, 4)]:
                send(send_a.at[p, base + r], recv_a.at[p, me], A + p, v, r)

        def away():
            send(send_a.at[p, my_g], recv_a.at[p, me], A + p, taker, lax.rem(ms, 4))

        unless(serves, away)

        def stay():
            recv_a[p, me] = send_a[p, my_g]

        pl.when(serves)(stay)

    def wait_sums(p):
        owner_only(lambda: got(recv_s.at[p, pl.ds(0, S * O - 1)], SM + p))
        other_only(lambda: got(recv_s.at[p, pl.ds(0, S * O)], SM + p))

    lane = lax.broadcasted_iota(jnp.int32, (ph, LANES), 1)
    sub = lax.broadcasted_iota(jnp.int32, (ph, LANES), 0)

    def length(p):
        wait_sums(p)
        total = recv_s[p, 0]
        for k in range(1, S * O):
            total = total + recv_s[p, k]
        total = jnp.broadcast_to(total, (ph, LANES))
        cross = jnp.sum(jnp.where(lane == sub, total, 0.0), axis=1, keepdims=True)
        square = jnp.sum(jnp.where(lane == sub + ph, total, 0.0), axis=1, keepdims=True)
        return cross / (square + EPSILON)

    def advance(factor, p, dst):
        for q in range(O):
            at = slice(q * chunk, (q + 1) * chunk)
            dst[:, at] = cur[:, at] - factor * recv_u[p, q].astype(F32)

    def serve(p, factor):
        mk("gotA")
        got(recv_a.at[p, pl.ds(0, N - 1)], A + p)
        mk("serve")
        if p == 0:
            def take():
                got(beta_two, BETA)
                got(inv.at[1], INV)

            unless(keeps, take)
            coef[...] = jnp.zeros(coef.shape, F32)
            coef[:, 0:kept] = beta_two[...]
        stack = []
        for v in range(V):
            val = recv_a[p, v].astype(F32)
            for s in range(1, S):
                val = val + recv_a[p, s * V + v].astype(F32)
            high = val.astype(BF16).astype(F32)
            stack += [high, val - high]
        found = dot(jnp.concatenate(stack, axis=0).astype(BF16), place_v[...])
        slots = jnp.zeros((ph, fit), F32)
        for v in range(V):
            both = found[2 * v * ph:(2 * v + 1) * ph] + found[(2 * v + 1) * ph:(2 * v + 2) * ph]
            slots = slots + marks_v[v:v + 1] * both
        slots = slots * inv_root
        if p > 0:
            slots = grad[...] - factor * slots
            coef[...] = coef[...] + factor * direct[p - 1].astype(F32)
        grad[...] = slots
        inner = slots - PENALTY * coef[...]
        ways = []
        for b in range(blocks):
            cut = slice(b * bsize, (b + 1) * bsize)
            ways.append(joined(dot(split(inner[:, cut]), inv[1, b], NT)).astype(BF16))
        way = jnp.concatenate(ways, axis=1)
        direct[p] = way
        way = way.astype(F32)
        spread = jnp.concatenate([way * marks_v[v:v + 1] for v in range(V)], axis=0).astype(BF16)
        back = dot(spread, place_v[...], NT).astype(BF16)
        for v in range(V):
            send_b[p, v] = back[v * ph:(v + 1) * ph]
        mk("sendB")
        for s in samps + [ms]:
            for v in all_var:
                send(send_b.at[p, v], recv_b.at[p, my_g], B + p, v, s)
        for s in samps:
            send(send_b.at[p, mv], recv_b.at[p, my_g], B + p, mv, s)
        recv_b[p, my_g] = send_b[p, mv]
        mk(None)

    def tell_direct(p):
        for s in samps:
            send(direct.at[p], recv_d.at[p], D + p, my_g, s)

        def away():
            send(direct.at[p], recv_d.at[p], D + p, my_g, ms)

        unless(keeps, away)

        def stay():
            recv_d[p] = direct[p]

        pl.when(keeps)(stay)

    def reduce(p):
        mk("gotC")
        got(recv_c.at[p, pl.ds(0, V - 1)], C + p)
        mk("sumC")
        val = recv_c[p, 0].astype(F32)
        for v in range(1, V):
            val = val + recv_c[p, v].astype(F32)
        low_u = (val * inv_root).astype(BF16)
        recv_u[p, my_q] = low_u

        def tell_update():
            for v in all_var:
                send(recv_u.at[p, my_q], recv_u.at[p, my_q], U + p, v, ms, UQ + p * O + my_q)

        def tell_sums():
            upd = low_u.astype(F32)
            now = cur[:, pl.ds(pl.multiple_of(my_q * chunk, chunk), chunk)]
            cross = jnp.sum(now * upd, axis=1, keepdims=True)
            square = jnp.sum(upd * upd, axis=1, keepdims=True)
            both = jnp.where(lane == sub, cross, jnp.where(lane == sub + ph, square, 0.0))
            slot = ms * O + my_q
            recv_s[p, slot] = jnp.sum(both, axis=0, keepdims=True)
            for s in samps + [ms]:
                for v in all_var:
                    send(recv_s.at[p, slot], recv_s.at[p, slot], SM + p, v, s)
            for s in samps:
                send(recv_s.at[p, slot], recv_s.at[p, slot], SM + p, mv, s)

        if p + 1 < PASSES:
            tell_update()
            tell_sums()
        else:
            tell_sums()
            tell_update()
        mk(None)

    def turn_rows(i, c):
        at = pl.ds(pl.multiple_of(i * turned, turned), turned)
        for j in range(width // turned):
            cut = slice(j * turned, (j + 1) * turned)
            xt_ref[cut, at] = x_ref[at, cut].T
        return c

    for n, (hh, ss) in enumerate(reversed(halves)):
        mk("idswait")
        got(ids_all.at[pl.ds(0, 3 if n == 0 else 4)], IQ + 2 * hh + ss)
        mk("idsproc")
        place_half(hh, ss)
        mk(None)
        if n == 0:
            pl.when(serves)(own_slots)
    factors = []
    for p in range(PASSES):
        mk("gather")
        send_gradient(p)
        mk("mid")
        if p == 0:
            mk("turn")
            lax.fori_loop(0, rows // turned, turn_rows, 0)
            mk("mid")
        if p == 1:
            mk("cmpA1")
            compact(3)
            mk("mid")
            got(recv_p.at[pl.ds(0, S - 1)], SC)
            val = recv_p[0]
            for s in range(1, S):
                val = val + recv_p[s]
            scores_out[...] = val * inv_root
        if p > 0:
            factors.append(length(p - 1))
        factor = factors[-1] if p else None
        mk(None)
        pl.when(serves)(functools.partial(serve, p, factor))
        mk("adv")
        if p > 0:
            advance(factor, p - 1, cur)
        if p < 2:
            mk("cmpB")
            if p == 0:
                build_pick()
            compact(0 if p == 0 else 4)
        mk("waitB")
        pl.when(serves)(lambda: got(recv_b.at[p, pl.ds(0, V - 1)], B + p))
        unless(serves, lambda: got(recv_b.at[p], B + p))
        mk("spread")
        way = jnp.concatenate([recv_b[p, g] for g in range(V)], axis=1)
        if p == 0:
            way = way.astype(F32)
            which = high_t[...]
            wide = jnp.concatenate([jnp.where(which == float(t), way, 0.0) for t in range(tiles)], axis=0)
            found = dot(wide.astype(BF16), low[...], NT).astype(BF16)
            for t in range(tiles):
                d_held[:, t * LANES:(t + 1) * LANES] = found[t * ph:(t + 1) * ph]
        mk("upd")

        for k, (v, q) in enumerate(owners):
            at = pl.ds(pl.multiple_of(q * chunk, chunk), chunk)
            if p == 0:
                send_c[p, q] = dot(d_held[...], xt_ref[:, at]).astype(BF16)
            else:
                send_c[p, q] = dot(way, xct_ref[:, at]).astype(BF16)
            if k < O - 1:
                send(send_c.at[p, q], recv_c.at[p, mv], C + p, v, ms)
            else:
                def away(q=q, v=v):
                    send(send_c.at[p, q], recv_c.at[p, mv], C + p, v, ms)

                other_only(away)

                def stay(q=q):
                    recv_c[p, mv] = send_c[p, q]

                owner_only(stay)
        pl.when(serves)(functools.partial(tell_direct, p))
        if p == 0:
            for s in samps:
                send(recv_p.at[ms], recv_p.at[ms], SC, mv, s)
        mk(None)
        if p == 0:
            mk("cmpC")
            compact(1)
            mk(None)
        owner_only(functools.partial(reduce, p))
        if p == 0:
            mk("cmpU")
            compact(2)
        mk("waitU")
        for k, (v, q) in enumerate(reversed(owners)):
            def arrive(q=q):
                got(recv_u.at[p, q], UQ + p * O + q)

            if k == 0:
                other_only(arrive)
            else:
                arrive()
            if p + 1 < PASSES:
                at = pl.ds(pl.multiple_of(q * chunk, chunk), chunk)
                left = PASSES - 2 - p
                new = dot(recv_u[p, q], x_ref[at, :] if left else xc_ref[at, :])
                total = part if left else part_c
                if k == 0:
                    total[...] = new
                else:
                    total[...] += new

    mk("fin")
    factors.append(length(PASSES - 1))
    factor = factors[-1]
    advance(factor, PASSES - 1, resid_out)

    coef_out[...] = jnp.zeros((ph, fit), F32)
    coef_out[:, 0:kept] = beta_v[...]
    val = coef_out[...]
    for p in range(PASSES):
        unless(keeps, functools.partial(lambda p: got(recv_d.at[p], D + p), p))
        val = val + factors[p] * recv_d[p].astype(F32)
    coef_out[...] = val
    mk("drain")

    sent(ids_all.at[pl.ds(0, V - 1)], IDS)
    sent(recv_p.at[pl.ds(0, S - 1)], SC)

    def drain_a(p):
        pl.when(serves)(lambda: sent(recv_a.at[p, pl.ds(0, V - 1)], A + p))
        unless(serves, lambda: sent(recv_a.at[p, pl.ds(0, V)], A + p))

    def drain_serve():
        for p in range(PASSES):
            sent(recv_a.at[p, pl.ds(0, N - 1)], B + p)
            pl.when(keeps)(functools.partial(lambda p: sent(blank.at[pl.ds(0, S - 1)], D + p), p))
            unless(keeps, functools.partial(lambda p: sent(blank, D + p), p))

    def drain_owner():
        for p in range(PASSES):
            sent(send_c.at[p, pl.ds(0, O - 1)], C + p)
            sent(recv_c.at[p, pl.ds(0, V - 1)], U + p)
            sent(recv_s.at[p, pl.ds(0, N - 1)], SM + p)

    def drain_other():
        for p in range(PASSES):
            sent(send_c.at[p], C + p)

    def drain_gives():
        sent(beta_v, BETA)
        sent(inv.at[0], INV)

    for p in range(PASSES):
        drain_a(p)
    pl.when(serves)(drain_serve)
    owner_only(drain_owner)
    pl.when(gives)(drain_gives)
    other_only(drain_other)


def on_device(geno, scale_index, scale_table, residual, beta_active, block_inverse, active_ids, admit_ids):
    V, S = lax.axis_size("var"), lax.axis_size("samp")
    N = V * S
    O = V // 4
    assert V % 8 == 0 and S >= 4
    rows, width = geno.shape
    ph = residual.shape[0]
    fit = active_ids.shape[0] + admit_ids.shape[0]
    pad = LANES * pl.cdiv(2 * fit // V, LANES)
    chunk = rows // O
    vmem = pl.BlockSpec(memory_space=pltpu.VMEM)
    hbm = pl.BlockSpec(memory_space=pl.ANY)
    n_send = 4 + 6 * PASSES
    n_recv = n_send + PASSES * O + O
    per_group = rows // scale_index.shape[0]
    out = pl.pallas_call(
        functools.partial(kernel, V, S, pad),
        out_shape=(pltpu.VMEM((ph, width), F32), pltpu.VMEM((ph, fit), F32), pltpu.VMEM((ph, rows), F32)),
        in_specs=[hbm] * 8,
        out_specs=(vmem, vmem, vmem),
        scratch_shapes=[
            pltpu.VMEM((rows, width), BF16),
            pltpu.VMEM((width, rows), BF16),
            pltpu.VMEM((width, V * pad), BF16),
            pltpu.VMEM((rows, V * pad), BF16),
            pltpu.VMEM((V * pad, rows), BF16),
            pltpu.VMEM((ph, V * pad), F32),
            pltpu.VMEM(scale_index.shape, jnp.int32),
            pltpu.SMEM(scale_table.shape, F32),
            pltpu.VMEM((ph, rows), F32),
            pltpu.VMEM(beta_active.shape, F32),
            pltpu.VMEM(block_inverse.shape, F32),
            pltpu.VMEM((1, active_ids.shape[0]), jnp.int32),
            pltpu.VMEM((1, admit_ids.shape[0]), jnp.int32),
            pltpu.VMEM(scale_index.shape, F32),
            pltpu.VMEM((ph, rows), BF16),
            pltpu.VMEM((ph, width), F32),
            pltpu.VMEM((LANES, V * pad), BF16),
            pltpu.VMEM((ph, V * pad), F32),
            pltpu.VMEM((V, fit), F32),
            pltpu.VMEM((pad, fit), BF16),
            pltpu.VMEM((fit, fit), BF16),
            pltpu.VMEM((2,) + block_inverse.shape, BF16),
            pltpu.VMEM(beta_active.shape, F32),
            pltpu.VMEM((V, 1, fit), jnp.int32),
            pltpu.VMEM((S, ph, fit), BF16),
            pltpu.VMEM((ph, width), BF16),
            pltpu.VMEM((ph, fit), F32),
            pltpu.VMEM((ph, fit), F32),
            pltpu.VMEM((PASSES, ph, fit), BF16),
            pltpu.VMEM((PASSES, V, ph, pad), BF16),
            pltpu.VMEM((PASSES, N, ph, pad), BF16),
            pltpu.VMEM((PASSES, V, ph, pad), BF16),
            pltpu.VMEM((PASSES, V, ph, pad), BF16),
            pltpu.VMEM((PASSES, O, ph, chunk), BF16),
            pltpu.VMEM((PASSES, V, ph, chunk), BF16),
            pltpu.VMEM((PASSES, O, ph, chunk), BF16),
            pltpu.VMEM((S, ph, width), F32),
            pltpu.VMEM((PASSES, N, 1, LANES), F32),
            pltpu.VMEM((PASSES, ph, fit), BF16),
            pltpu.SemaphoreType.DMA((rows // (2 * per_group),)),
            pltpu.SemaphoreType.DMA((7,)),
            pltpu.SemaphoreType.DMA((n_send,)),
            pltpu.SemaphoreType.DMA((n_recv,)),
        ],
        compiler_params=pltpu.CompilerParams(
            collective_id=0, has_side_effects=True, vmem_limit_bytes=60 * 1024 * 1024
        ),
    )(geno, scale_index, scale_table, residual, beta_active, block_inverse, active_ids[None], admit_ids[None])

    def hand_out(*refs):
        half = len(refs) // 2
        for a, b in zip(refs[:half], refs[half:]):
            b[...] = a[...]

    return pl.pallas_call(
        hand_out, out_shape=tuple(jax.ShapeDtypeStruct(o.shape, o.dtype) for o in out),
        in_specs=[vmem] * 3, out_specs=(vmem,) * 3,
        compiler_params=pltpu.CompilerParams(vmem_limit_bytes=1024 * 1024),
    )(*out)


def solution(mesh):
    placed = (
        P("samp", "var"), P("samp", "var"), P(), P(None, "samp"), P(None, "var"),
        P("var", None, None), P("var"), P("var"),
    )
    return jax.shard_map(
        on_device, mesh=mesh, in_specs=placed,
        out_specs=(P(None, "var"), P(None, "var"), P(None, "samp")), check_vma=False,
    )
```
